32 devices in a mesh: outer: 4 (over y, x), inner: 8 (over z, core).
Axes of the slice: x: 2, y: 2, z: 4, core: 2. Of those that a mesh axis runs over, the one named last changes fastest.
Arguments:
- activations: bfloat16 [4096, 128], P(('outer', 'inner')), may hold values from -6 to 6
- out_grads: bfloat16 [4096, 8192], P(('outer', 'inner')), may hold values from -6 to 6
- momentum: float32 [8192, 128], P(('outer', 'inner')), may hold values from -6 to 6
- first_exp: int32 [8192], replicated, may hold values from -3 to -1
- second_exp: int32 [8192], replicated, may hold values from -2 to 2
- third_exp: int32 [8192], replicated, may hold values from -7 to -5
- signs: int32 [2, 128], replicated, may hold values from 0 to 1
Outputs:
- new_momentum: float32 [8192, 128], P(('outer', 'inner'))
- update: bfloat16 [128, 8192], replicated
The draws below stay inside these ranges and needn't reach their ends.
All inputs are finite; a program needn't handle non-finite values.
Results may differ from the reference program's by a relative error of at most 0.017.
Values may be sent and summed in bfloat16 or wider, within the bound.
No kernel may reach another device: no remote copies, remote signals or barrier semaphores. Data moves between devices by JAX's collectives and lax.ppermute only.
A program may use at most 64 MiB of HBM per device.

```python
import jax
import jax.numpy as jnp
from jax import lax

D = 8192
ROWS = 128
TOK_DEV = 128
BLOCK = 128
BLOCKS = 8192
TOKENS = 4096
N_OUTER = 4
N_INNER = 8
DEVICES = 32


def with_ends(entries, key, smallest, top_value):
    shape = entries.shape
    spot = [jax.random.randint(jax.random.fold_in(key, axis), (), 0, shape[axis]) for axis in range(len(shape))]
    entries = entries.at[tuple(spot)].set(smallest)
    longest = shape.index(max(shape))
    spot[longest] = (spot[longest] + 1) % shape[longest]
    return entries.at[tuple(spot)].set(top_value)


def level_of(key, dims, split, least, largest):
    gain, own = 1.0, jax.random.fold_in(key, 6)
    for axis_at, parts in split:
        draws = jnp.exp(jax.random.uniform(jax.random.fold_in(own, axis_at), (parts,), jnp.float32, least / len(split), largest / len(split)))
        gain = gain * jnp.repeat(draws, dims[axis_at] // parts).reshape([-1 if axis == axis_at else 1 for axis in range(len(dims))])
    return gain


def gaussian(key, extent, width, reach, shards=(), kind=jnp.bfloat16):
    array = width * jax.random.normal(key, extent, jnp.float32)
    if shards:
        array = array * level_of(key, extent, shards, -0.22, 0.18)
    return jnp.clip(array, -reach, reach).astype(kind)


def setup_inputs(seed: int = 0) -> dict:
    seeds = jax.random.split(jax.random.key(seed), 8)
    return {
        "activations": gaussian(seeds[0], (TOKENS, ROWS), 1.0, 6.0, ((0, 32),)),
        "out_grads": gaussian(seeds[1], (TOKENS, D), 1.0, 6.0, ((0, 32),)),
        "momentum": gaussian(seeds[2], (BLOCKS, BLOCK), 1.0, 6.0, ((0, 32),), jnp.float32),
        "first_exp": with_ends(jax.random.randint(seeds[3], (BLOCKS,), -3, 0), jax.random.fold_in(seeds[3], 1), -3, -1).astype(jnp.int32),
        "second_exp": with_ends(jax.random.randint(seeds[4], (BLOCKS,), -2, 3), jax.random.fold_in(seeds[4], 1), -2, 2).astype(jnp.int32),
        "third_exp": with_ends(jax.random.randint(seeds[5], (BLOCKS,), -7, -4), jax.random.fold_in(seeds[5], 1), -7, (-4) - 1).astype(jnp.int32),
        "signs": with_ends(jax.random.randint(seeds[6], (2, BLOCK), 0, 2), jax.random.fold_in(seeds[6], 1), 0, 1).astype(jnp.int32),
    }


quant_limit = 127.0
momentum_decay = 0.9
step_size = 0.5

def hadamard_matrix(order):
    position = jnp.arange(order, dtype=jnp.int32)
    common = jnp.bitwise_and(position[:, None], position[None, :])
    parity = jnp.zeros((order, order), jnp.int32)
    for shift_by in range(order.bit_length() - 1):
        parity = parity + jnp.bitwise_and(jnp.right_shift(common, shift_by), 1)
    return 1.0 - 2.0 * jnp.bitwise_and(parity, 1).astype(jnp.float32)

def rotation(sign_bits):
    order = sign_bits.shape[0]
    flips = 1.0 - 2.0 * sign_bits.astype(jnp.float32)
    return flips[:, None] * hadamard_matrix(order) / jnp.sqrt(jnp.float32(order))

def reference(activations, out_grads, momentum, first_exp, second_exp, third_exp, signs):
    high = lax.Precision.HIGHEST
    first_rot = rotation(signs[0])
    second_rot = rotation(signs[1])
    count_blocks = ROWS * D // BLOCK
    acts = activations.reshape(N_OUTER, N_INNER, TOK_DEV, ROWS)
    grads = out_grads.reshape(N_OUTER, N_INNER, TOK_DEV, D)
    first_down = jnp.exp2(-first_exp.astype(jnp.float32))[:, None]
    shift_scale = jnp.exp2((first_exp - second_exp).astype(jnp.float32))[:, None]

    def replica(inputs, outgrad):
        grad = lax.dot_general(inputs, outgrad, (((0,), (0,)), ((), ())), preferred_element_type=jnp.float32)
        rotated = jnp.dot(grad.reshape(count_blocks, BLOCK), first_rot, precision=high)
        return jnp.clip(rotated * first_down, -quant_limit, quant_limit).astype(jnp.bfloat16)

    def add_inner(accum, item):
        return (accum + replica(item[0], item[1]).astype(jnp.float32), None)

    def add_outer(total, item):
        start = jnp.zeros((count_blocks, BLOCK), jnp.float32)
        inner_total, unused = lax.scan(add_inner, start, item)
        requant = jnp.clip(inner_total * shift_scale, -quant_limit, quant_limit).astype(jnp.bfloat16)
        return (total + requant.astype(jnp.float32), None)
    total, unused = lax.scan(add_outer, jnp.zeros((count_blocks, BLOCK), jnp.float32), (acts, grads))
    second_up = jnp.exp2(second_exp.astype(jnp.float32))[:, None]
    mean_grad = jnp.dot(total * second_up, first_rot.T, precision=high) / DEVICES
    new_momentum = momentum_decay * momentum + mean_grad
    rotated_step = jnp.dot(-step_size * new_momentum, second_rot, precision=high)
    third_down = jnp.exp2(-third_exp.astype(jnp.float32))[:, None]
    quant_third = jnp.clip(rotated_step * third_down, -quant_limit, quant_limit).astype(jnp.bfloat16)
    third_up = jnp.exp2(third_exp.astype(jnp.float32))[:, None]
    restored = jnp.dot(quant_third.astype(jnp.float32) * third_up, second_rot.T, precision=high)
    update = restored.astype(jnp.bfloat16).reshape(ROWS, D)
    return (new_momentum, update)
```

```python
import jax
import jax.numpy as jnp
from jax import lax
from jax.experimental import pallas as pl
from jax.experimental.pallas import tpu as pltpu
from jax.sharding import PartitionSpec as P


quant_limit = 127.0
momentum_decay = 0.9
step_size = 0.5


def hadamard_matrix(order):
    position = jnp.arange(order, dtype=jnp.int32)
    common = jnp.bitwise_and(position[:, None], position[None, :])
    parity = jnp.zeros((order, order), jnp.int32)
    for shift_by in range(order.bit_length() - 1):
        parity = parity + jnp.bitwise_and(jnp.right_shift(common, shift_by), 1)
    return 1.0 - 2.0 * jnp.bitwise_and(parity, 1).astype(jnp.float32)


def rotation(sign_bits):
    order = sign_bits.shape[0]
    flips = 1.0 - 2.0 * sign_bits.astype(jnp.float32)
    return flips[:, None] * hadamard_matrix(order) / jnp.sqrt(jnp.float32(order))


def collect(pieces):
    grouped = lax.all_gather(pieces[None], "outer", axis=0, tiled=True)
    spread = lax.all_gather(grouped, "inner", axis=1, tiled=True)
    return spread.reshape(-1, pieces.shape[1])


def general(activations, out_grads, momentum, first_exp, second_exp, third_exp, signs):
    high = lax.Precision.HIGHEST
    outer_count = lax.axis_size("outer")
    inner_count = lax.axis_size("inner")
    outer_place = lax.axis_index("outer")
    inner_place = lax.axis_index("inner")
    device_count = outer_count * inner_count
    first_rot = rotation(signs[0])
    second_rot = rotation(signs[1])
    grad = lax.dot_general(
        activations, out_grads, (((0,), (0,)), ((), ())), preferred_element_type=jnp.float32
    )
    slab_shape = grad.shape
    order = first_rot.shape[0]
    count_blocks = grad.size // order
    shard_rows = count_blocks // device_count
    rotated = jnp.dot(grad.reshape(count_blocks, order), first_rot, precision=high)
    first_down = jnp.exp2(-first_exp.astype(jnp.float32))[:, None]
    quant_first = jnp.clip(rotated * first_down, -quant_limit, quant_limit).astype(jnp.bfloat16)
    grouped = quant_first.astype(jnp.float32).reshape(outer_count, inner_count * shard_rows, order)
    inner_total = lax.psum_scatter(
        grouped.astype(jnp.bfloat16), "inner", scatter_dimension=1, tiled=True
    ).astype(jnp.float32)
    first_grid = first_exp.reshape(outer_count, inner_count, shard_rows)
    second_grid = second_exp.reshape(outer_count, inner_count, shard_rows)
    third_grid = third_exp.reshape(outer_count, inner_count, shard_rows)
    first_here = lax.dynamic_index_in_dim(first_grid, inner_place, 1, keepdims=False)
    second_here = lax.dynamic_index_in_dim(second_grid, inner_place, 1, keepdims=False)
    shift_scale = jnp.exp2((first_here - second_here).astype(jnp.float32))[:, :, None]
    requant = jnp.clip(inner_total * shift_scale, -quant_limit, quant_limit).astype(jnp.bfloat16)
    total = lax.psum_scatter(
        requant.astype(jnp.float32).astype(jnp.bfloat16), "outer", scatter_dimension=0, tiled=True
    ).astype(jnp.float32)[0]
    second_mine = lax.dynamic_index_in_dim(second_here, outer_place, 0, keepdims=False)
    second_up = jnp.exp2(second_mine.astype(jnp.float32))[:, None]
    mean_grad = jnp.dot(total * second_up, first_rot.T, precision=high) / device_count
    new_momentum = momentum_decay * momentum + mean_grad
    third_row = lax.dynamic_index_in_dim(third_grid, outer_place, 0, keepdims=False)
    third_mine = lax.dynamic_index_in_dim(third_row, inner_place, 0, keepdims=False)
    rotated_step = jnp.dot(-step_size * new_momentum, second_rot, precision=high)
    third_down = jnp.exp2(-third_mine.astype(jnp.float32))[:, None]
    quant_third = jnp.clip(rotated_step * third_down, -quant_limit, quant_limit).astype(
        jnp.bfloat16
    )
    third_up = jnp.exp2(third_mine.astype(jnp.float32))[:, None]
    restored = jnp.dot(quant_third.astype(jnp.float32) * third_up, second_rot.T, precision=high)
    update = collect(restored.astype(jnp.bfloat16)).reshape(slab_shape)
    return (new_momentum, update)


def log2(count):
    return count.bit_length() - 1


def power_of_two(count):
    return count > 0 and count & (count - 1) == 0


class Plan:
    def __init__(self, activations, out_grads, signs, outer, inner):
        self.outer, self.inner = outer, inner
        self.levels = inner // 2
        self.tokens, self.rows = activations.shape
        self.order = signs.shape[1]
        self.width = out_grads.shape[1]
        self.chunks = self.width // self.order
        self.own_rows = self.rows // (outer * inner)
        self.seg_rows = outer * self.own_rows
        self.slab_rows = self.levels * self.own_rows

    def fits(self):
        return (
            all(power_of_two(n) for n in (self.outer, self.inner, self.rows, self.chunks))
            and self.levels >= 2
            and self.own_rows * self.outer * self.inner == self.rows
            and self.seg_rows == 16
            and self.slab_rows == 16
            and self.order == 128
            and 2 * self.chunks == self.order
        )


def places():
    outer_place = lax.axis_index("outer")
    inner_place = lax.axis_index("inner")
    return outer_place, inner_place >> 1, inner_place & 1


def iota(shape, axis):
    return lax.broadcasted_iota(jnp.int32, shape, axis)


def pick(plan, row_of, scale):
    count = row_of.shape[0]
    lines = scale.shape[0]
    line = iota((count, lines), 1)
    row_of = jnp.broadcast_to(row_of, (count, lines))
    even = jnp.where(row_of == 2 * line, 1.0, 0.0).astype(jnp.bfloat16)
    odd = jnp.where(row_of == 2 * line + 1, 1.0, 0.0).astype(jnp.bfloat16)
    table = scale.astype(jnp.bfloat16)
    half = plan.chunks
    low = jnp.dot(even, table[:, :half], preferred_element_type=jnp.float32)
    high = jnp.dot(odd, table[:, half:], preferred_element_type=jnp.float32)
    return low + high


def two_terms(values):
    high = values.astype(jnp.bfloat16)
    low = (values - high.astype(jnp.float32)).astype(jnp.bfloat16)
    return jnp.concatenate([high, low], axis=1)


def clip_round(values):
    return jnp.clip(values, -quant_limit, quant_limit).astype(jnp.bfloat16)


def front(plan, span, mine, activations, out_grads, first_exp, flips):
    first_chunk, chunk_count = span
    group = min(8, chunk_count)
    groups = chunk_count // group
    half_rows = plan.rows // 2
    seg = plan.seg_rows
    wide = group * plan.order

    def kernel(acts_ref, grads_ref, exp_ref, flips_ref, *refs):
        outs, (grads_vmem, sems) = refs[:-2], refs[-2:]

        def copy(step):
            at = (first_chunk + step * group) * plan.order
            return pltpu.make_async_copy(
                grads_ref.at[:, pl.ds(at, wide)], grads_vmem.at[step], sems.at[step]
            )

        for step in range(groups):
            copy(step).start()
        outer_place, level, core = places()
        keeper = core if mine else 1 - core
        index = iota((half_rows, 1), 0)
        own = index & (plan.own_rows - 1)
        hop_outer = (index >> log2(plan.own_rows)) & (plan.outer - 1)
        hop_level = index >> log2(seg)
        inner_of = 2 * (level ^ hop_level) + keeper
        row_of = ((outer_place ^ hop_outer) * plan.inner + inner_of) * plan.own_rows + own
        chooser = jnp.where(
            iota((half_rows, plan.rows), 1) == jnp.broadcast_to(row_of, (half_rows, plan.rows)),
            1.0,
            0.0,
        ).astype(jnp.bfloat16)
        acts = lax.dot_general(
            chooser, acts_ref[...], (((1,), (1,)), ((), ())), preferred_element_type=jnp.float32
        ).astype(jnp.bfloat16)
        root = 1.0 / (plan.order**0.5)
        down = pick(plan, row_of, jnp.exp2(-exp_ref[...].astype(jnp.float32))) * root
        turn = jnp.concatenate([flips_ref[...], flips_ref[...]], axis=0)
        for step in range(groups):
            copy(step).wait()
            grad = jnp.dot(acts, grads_vmem[step], preferred_element_type=jnp.float32)
            stacked = jnp.concatenate(
                [grad[:, c * plan.order : (c + 1) * plan.order] for c in range(group)], axis=0
            )
            rotated = jnp.dot(two_terms(stacked), turn, preferred_element_type=jnp.float32)
            for c in range(group):
                at = first_chunk + step * group + c
                part = rotated[c * half_rows : (c + 1) * half_rows] * down[:, at : at + 1]
                part = clip_round(part)
                for hop in range(plan.levels):
                    row = (step * group + c) * seg
                    outs[hop][pl.ds(row, seg), :] = part[hop * seg : (hop + 1) * seg]

    piece = jax.ShapeDtypeStruct((chunk_count * seg, plan.order), jnp.bfloat16)
    return pl.pallas_call(
        kernel,
        out_shape=[piece] * plan.levels,
        in_specs=[
            pl.BlockSpec(memory_space=pltpu.VMEM),
            pl.BlockSpec(memory_space=pl.ANY),
            pl.BlockSpec(memory_space=pltpu.VMEM),
            pl.BlockSpec(memory_space=pltpu.VMEM),
        ],
        out_specs=[pl.BlockSpec(memory_space=pltpu.VMEM)] * plan.levels,
        scratch_shapes=[
            pltpu.VMEM((groups, plan.tokens, wide), jnp.bfloat16),
            pltpu.SemaphoreType.DMA((groups,)),
        ],
        name="front_mine" if mine else "front_theirs",
    )(activations, out_grads, first_exp, flips)


def join_cores(plan, span, ours, theirs):
    def kernel(*refs):
        count = plan.levels
        for hop in range(count):
            one, two, out = refs[hop], refs[count + hop], refs[2 * count + hop]
            out[...] = (one[...].astype(jnp.float32) + two[...].astype(jnp.float32)).astype(
                jnp.bfloat16
            )

    piece = jax.ShapeDtypeStruct(ours[0].shape, jnp.bfloat16)
    return pl.pallas_call(kernel, out_shape=[piece] * plan.levels, name="join_cores")(
        *ours, *theirs
    )


def requantize(plan, span, first_exp, second_exp, parts):
    first_chunk, chunk_count = span
    seg = plan.seg_rows
    group = min(16, chunk_count)
    size = group * seg

    def kernel(first_ref, second_ref, *refs):
        ins, outs = refs[: plan.levels], refs[plan.levels :]
        outer_place, level, core = places()
        index = iota((seg, 1), 0)
        own = index & (plan.own_rows - 1)
        hop = index >> log2(plan.own_rows)
        inner_of = 2 * level + core
        row_of = ((outer_place ^ hop) * plan.inner + inner_of) * plan.own_rows + own
        shift = pick(plan, row_of, jnp.exp2((first_ref[...] - second_ref[...]).astype(jnp.float32)))
        here, there = iota((size, size), 0), iota((size, size), 1)
        source = (here & (group - 1)) * seg + (here >> log2(group))
        order = jnp.where(there == source, 1.0, 0.0).astype(jnp.bfloat16)
        for step in range(chunk_count // group):
            rows = pl.ds(step * size, size)
            total = ins[0][rows, :].astype(jnp.float32)
            for other in ins[1:]:
                total = total + other[rows, :].astype(jnp.float32)
            scaled = jnp.concatenate(
                [
                    total[c * seg : (c + 1) * seg] * shift[:, at : at + 1]
                    for c, at in enumerate(range(first_chunk + step * group, first_chunk + (step + 1) * group))
                ],
                axis=0,
            )
            moved = jnp.dot(order, clip_round(scaled), preferred_element_type=jnp.float32)
            moved = moved.astype(jnp.bfloat16)
            for m in range(seg):
                out, row = outs[m // plan.own_rows], (m % plan.own_rows) * chunk_count + step * group
                out[pl.ds(row, group), :] = moved[m * group : (m + 1) * group]

    piece = jax.ShapeDtypeStruct((plan.own_rows * chunk_count, plan.order), jnp.bfloat16)
    return pl.pallas_call(kernel, out_shape=[piece] * plan.outer, name="requantize")(
        first_exp, second_exp, *parts
    )


def owner(plan, span, second_exp, third_exp, flips_one, flips_two, momentum, parts):
    first_chunk, chunk_count = span
    own_rows, order = plan.own_rows, plan.order
    devices = plan.outer * plan.inner

    def kernel(second_ref, third_ref, one_ref, two_ref, momentum_ref, *refs):
        ins, (moment_out, update_out) = refs[: plan.outer], refs[plan.outer :]
        outer_place, level, core = places()
        first_row = (outer_place * plan.inner + 2 * level + core) * own_rows
        row_of = first_row + iota((own_rows, 1), 0)
        diagonal = iota((chunk_count, chunk_count), 0) == iota((chunk_count, chunk_count), 1)

        def column(table):
            chosen = pick(plan, row_of, table)[:, first_chunk : first_chunk + chunk_count]
            return jnp.concatenate(
                [
                    jnp.sum(jnp.where(diagonal, chosen[k : k + 1], 0.0), axis=1, keepdims=True)
                    for k in range(own_rows)
                ],
                axis=0,
            )

        second = second_ref[...].astype(jnp.float32)
        third = third_ref[...].astype(jnp.float32)
        up, third_down, third_up = (column(jnp.exp2(e)) for e in (second, -third, third))
        root = 1.0 / (order**0.5)
        total = ins[0][...].astype(jnp.float32)
        for other in ins[1:]:
            total = total + other[...].astype(jnp.float32)
        one, two = one_ref[...], two_ref[...]
        back = lax.dot_general(
            two_terms(total * up),
            jnp.concatenate([one, one], axis=1),
            (((1,), (1,)), ((), ())),
            preferred_element_type=jnp.float32,
        )
        before = jnp.concatenate(
            [
                momentum_ref[pl.ds(k * plan.chunks + first_chunk, chunk_count), :]
                for k in range(own_rows)
            ],
            axis=0,
        )
        moment = momentum_decay * before + back * (root / devices)
        moment_out[...] = moment
        turned = jnp.dot(
            two_terms(-step_size * moment),
            jnp.concatenate([two, two], axis=0),
            preferred_element_type=jnp.float32,
        )
        quant = clip_round(turned * (third_down * root))
        restored = lax.dot_general(
            quant, two, (((1,), (1,)), ((), ())), preferred_element_type=jnp.float32
        )
        update_out[...] = (restored * (third_up * root)).astype(jnp.bfloat16)

    shape = (own_rows * chunk_count, order)
    return pl.pallas_call(
        kernel,
        out_shape=[
            jax.ShapeDtypeStruct(shape, jnp.float32),
            jax.ShapeDtypeStruct(shape, jnp.bfloat16),
        ],
        name="owner",
    )(second_exp, third_exp, flips_one, flips_two, momentum, *parts)


def half_slab(plan, span, parts):
    first_chunk, chunk_count = span
    own_rows, rows = plan.own_rows, plan.slab_rows
    group = min(16, chunk_count)
    size = group * rows

    def kernel(*refs):
        ins, out = refs[:-1], refs[-1]
        outer_place, level, core = places()
        here, there = iota((size, size), 0), iota((size, size), 1)
        row = here & (rows - 1)
        hop = (row >> log2(own_rows)) ^ level
        source = (hop * own_rows + (row & (own_rows - 1))) * group + (here >> log2(rows))
        order = jnp.where(there == source, 1.0, 0.0).astype(jnp.bfloat16)
        for step in range(chunk_count // group):
            block = jnp.concatenate(
                [
                    part[pl.ds(k * chunk_count + step * group, group), :]
                    for part in ins
                    for k in range(own_rows)
                ],
                axis=0,
            )
            moved = jnp.dot(order, block, preferred_element_type=jnp.float32).astype(jnp.bfloat16)
            for c in range(group):
                at = (step * group + c) * plan.order
                out[:, pl.ds(at, plan.order)] = moved[c * rows : (c + 1) * rows]

    shape = jax.ShapeDtypeStruct((rows, chunk_count * plan.order), jnp.bfloat16)
    return pl.pallas_call(kernel, out_shape=shape, name="half_slab")(*parts)


def place_slabs(plan, ours, theirs):
    spans = plan.spans

    def kernel(*refs):
        (out, sems), ins = refs[-2:], refs[:-2]
        outer_place, level, core = places()
        copies = []
        for n, (first_chunk, chunk_count) in enumerate(spans):
            for side in range(2):
                keeper = core if side == 0 else 1 - core
                for hop in range(plan.outer):
                    at = (n * 2 + side) * plan.outer + hop
                    row = ((outer_place ^ hop) * 2 + keeper) * plan.slab_rows
                    copies.append(
                        pltpu.make_async_copy(
                            ins[at],
                            out.at[
                                pl.ds(row, plan.slab_rows),
                                pl.ds(first_chunk * plan.order, chunk_count * plan.order),
                            ],
                            sems.at[at],
                        )
                    )
        for copy in copies:
            copy.start()
        for copy in copies:
            copy.wait()

    flat = [piece for n in range(len(spans)) for side in (ours[n], theirs[n]) for piece in side]
    return pl.pallas_call(
        kernel,
        out_shape=jax.ShapeDtypeStruct((plan.rows, plan.width), jnp.bfloat16),
        in_specs=[pl.BlockSpec(memory_space=pl.ANY)] * len(flat),
        out_specs=pl.BlockSpec(memory_space=pl.ANY),
        scratch_shapes=[pltpu.SemaphoreType.DMA((len(flat),))],
        name="place_slabs",
    )(*flat)


def send(plan, value, target_of):
    pairs = []
    for o in range(plan.outer):
        for z in range(plan.levels):
            for c in range(2):
                to, tz, tc = target_of(o, z, c)
                pairs.append((o * plan.inner + 2 * z + c, to * plan.inner + 2 * tz + tc))
    return lax.ppermute(value, ("outer", "inner"), pairs)


def swap_cores(plan, value):
    return send(plan, value, lambda o, z, c: (o, z, 1 - c))


def over_levels(plan, value, hop):
    return send(plan, value, lambda o, z, c: (o, z ^ hop, c))


def over_outer(plan, value, hop):
    return send(plan, value, lambda o, z, c: (o ^ hop, z, c))


def to_band(plan, value, hop):
    band = plan.levels // 2
    return send(
        plan, value, lambda o, z, c: (o, (2 * (z & (band - 1)) + c) ^ hop, z // band)
    )


def stream(plan, span, tables, activations, out_grads, momentum):
    first_exp, second_exp, third_exp, flips_one, flips_two = tables
    theirs = front(plan, span, False, activations, out_grads, first_exp, flips_one)
    theirs = [swap_cores(plan, piece) for piece in theirs]
    ours = front(plan, span, True, activations, out_grads, first_exp, flips_one)
    joined = join_cores(plan, span, ours, theirs)
    parts = [joined[0]] + [over_levels(plan, joined[hop], hop) for hop in range(1, plan.levels)]
    parts = requantize(plan, span, first_exp, second_exp, parts)
    parts = [parts[0]] + [over_outer(plan, parts[hop], hop) for hop in range(1, plan.outer)]
    moment, update = owner(plan, span, second_exp, third_exp, flips_one, flips_two, momentum, parts)
    band = [to_band(plan, update, hop) for hop in range(plan.levels)]
    slab = half_slab(plan, span, band)
    ours = [slab] + [over_outer(plan, slab, hop) for hop in range(1, plan.outer)]
    theirs = [swap_cores(plan, piece) for piece in ours]
    return moment, ours, theirs


def on_device(activations, out_grads, momentum, first_exp, second_exp, third_exp, signs):
    plan = Plan(activations, out_grads, signs, lax.axis_size("outer"), lax.axis_size("inner"))
    if not plan.fits():
        return general(activations, out_grads, momentum, first_exp, second_exp, third_exp, signs)
    plan.spans = split_chunks(plan.chunks)
    flips = 1.0 - 2.0 * signs.astype(jnp.float32)
    turns = (flips[:, :, None] * hadamard_matrix(plan.order)[None]).astype(jnp.bfloat16)
    exps = [e.reshape(-1, plan.order) for e in (first_exp, second_exp, third_exp)]
    tables = (*exps, turns[0], turns[1])
    done = [stream(plan, span, tables, activations, out_grads, momentum) for span in plan.spans]
    moments = [d[0].reshape(plan.own_rows, -1, plan.order) for d in done]
    new_momentum = jnp.concatenate(moments, axis=1).reshape(momentum.shape)
    update = place_slabs(plan, [d[1] for d in done], [d[2] for d in done])
    return (new_momentum, update)


def split_chunks(chunks):
    return [(0, chunks)]


def solution(mesh):
    in_specs = (
        P(("outer", "inner"), None),
        P(("outer", "inner"), None),
        P(("outer", "inner"), None),
        P(),
        P(),
        P(),
        P(),
    )
    out_specs = (P(("outer", "inner"), None), P())
    return jax.shard_map(
        on_device, mesh=mesh, in_specs=in_specs, out_specs=out_specs, check_vma=False
    )
```

```python
import jax
import jax.numpy as jnp
from jax import lax
from jax.experimental import pallas as pl
from jax.experimental.pallas import tpu as pltpu
from jax.sharding import PartitionSpec as P


quant_limit = 127.0
momentum_decay = 0.9
step_size = 0.5


def hadamard_matrix(order):
    position = jnp.arange(order, dtype=jnp.int32)
    common = jnp.bitwise_and(position[:, None], position[None, :])
    parity = jnp.zeros((order, order), jnp.int32)
    for shift_by in range(order.bit_length() - 1):
        parity = parity + jnp.bitwise_and(jnp.right_shift(common, shift_by), 1)
    return 1.0 - 2.0 * jnp.bitwise_and(parity, 1).astype(jnp.float32)


def rotation(sign_bits):
    order = sign_bits.shape[0]
    flips = 1.0 - 2.0 * sign_bits.astype(jnp.float32)
    return flips[:, None] * hadamard_matrix(order) / jnp.sqrt(jnp.float32(order))


def collect(pieces):
    grouped = lax.all_gather(pieces[None], "outer", axis=0, tiled=True)
    spread = lax.all_gather(grouped, "inner", axis=1, tiled=True)
    return spread.reshape(-1, pieces.shape[1])


def general(activations, out_grads, momentum, first_exp, second_exp, third_exp, signs):
    high = lax.Precision.HIGHEST
    outer_count = lax.axis_size("outer")
    inner_count = lax.axis_size("inner")
    outer_place = lax.axis_index("outer")
    inner_place = lax.axis_index("inner")
    device_count = outer_count * inner_count
    first_rot = rotation(signs[0])
    second_rot = rotation(signs[1])
    grad = lax.dot_general(
        activations, out_grads, (((0,), (0,)), ((), ())), preferred_element_type=jnp.float32
    )
    slab_shape = grad.shape
    order = first_rot.shape[0]
    count_blocks = grad.size // order
    shard_rows = count_blocks // device_count
    rotated = jnp.dot(grad.reshape(count_blocks, order), first_rot, precision=high)
    first_down = jnp.exp2(-first_exp.astype(jnp.float32))[:, None]
    quant_first = jnp.clip(rotated * first_down, -quant_limit, quant_limit).astype(jnp.bfloat16)
    grouped = quant_first.astype(jnp.float32).reshape(outer_count, inner_count * shard_rows, order)
    inner_total = lax.psum_scatter(
        grouped.astype(jnp.bfloat16), "inner", scatter_dimension=1, tiled=True
    ).astype(jnp.float32)
    first_grid = first_exp.reshape(outer_count, inner_count, shard_rows)
    second_grid = second_exp.reshape(outer_count, inner_count, shard_rows)
    third_grid = third_exp.reshape(outer_count, inner_count, shard_rows)
    first_here = lax.dynamic_index_in_dim(first_grid, inner_place, 1, keepdims=False)
    second_here = lax.dynamic_index_in_dim(second_grid, inner_place, 1, keepdims=False)
    shift_scale = jnp.exp2((first_here - second_here).astype(jnp.float32))[:, :, None]
    requant = jnp.clip(inner_total * shift_scale, -quant_limit, quant_limit).astype(jnp.bfloat16)
    total = lax.psum_scatter(
        requant.astype(jnp.float32).astype(jnp.bfloat16), "outer", scatter_dimension=0, tiled=True
    ).astype(jnp.float32)[0]
    second_mine = lax.dynamic_index_in_dim(second_here, outer_place, 0, keepdims=False)
    second_up = jnp.exp2(second_mine.astype(jnp.float32))[:, None]
    mean_grad = jnp.dot(total * second_up, first_rot.T, precision=high) / device_count
    new_momentum = momentum_decay * momentum + mean_grad
    third_row = lax.dynamic_index_in_dim(third_grid, outer_place, 0, keepdims=False)
    third_mine = lax.dynamic_index_in_dim(third_row, inner_place, 0, keepdims=False)
    rotated_step = jnp.dot(-step_size * new_momentum, second_rot, precision=high)
    third_down = jnp.exp2(-third_mine.astype(jnp.float32))[:, None]
    quant_third = jnp.clip(rotated_step * third_down, -quant_limit, quant_limit).astype(
        jnp.bfloat16
    )
    third_up = jnp.exp2(third_mine.astype(jnp.float32))[:, None]
    restored = jnp.dot(quant_third.astype(jnp.float32) * third_up, second_rot.T, precision=high)
    update = collect(restored.astype(jnp.bfloat16)).reshape(slab_shape)
    return (new_momentum, update)


def vmem(mebibytes):
    return pltpu.CompilerParams(vmem_limit_bytes=mebibytes * 1024 * 1024)


def log2(count):
    return count.bit_length() - 1


def power_of_two(count):
    return count > 0 and count & (count - 1) == 0


class Plan:
    def __init__(self, activations, out_grads, signs, outer, inner):
        self.outer, self.inner = outer, inner
        self.levels = inner // 2
        self.tokens, self.rows = activations.shape
        self.order = signs.shape[1]
        self.width = out_grads.shape[1]
        self.chunks = self.width // self.order
        self.own_rows = self.rows // (outer * inner)
        self.seg_rows = outer * self.own_rows
        self.slab_rows = self.levels * self.own_rows

    def fits(self):
        return (
            all(power_of_two(n) for n in (self.outer, self.inner, self.rows, self.chunks))
            and self.levels >= 2
            and self.own_rows * self.outer * self.inner == self.rows
            and self.seg_rows == 16
            and self.slab_rows == 16
            and self.order == 128
            and 2 * self.chunks == self.order
        )


def places():
    outer_place = lax.axis_index("outer")
    inner_place = lax.axis_index("inner")
    return outer_place, inner_place >> 1, inner_place & 1


def iota(shape, axis):
    return lax.broadcasted_iota(jnp.int32, shape, axis)


def pick(plan, row_of, scale):
    count = row_of.shape[0]
    lines = scale.shape[0]
    line = iota((count, lines), 1)
    row_of = jnp.broadcast_to(row_of, (count, lines))
    even = jnp.where(row_of == 2 * line, 1.0, 0.0).astype(jnp.bfloat16)
    odd = jnp.where(row_of == 2 * line + 1, 1.0, 0.0).astype(jnp.bfloat16)
    table = scale.astype(jnp.bfloat16)
    half = plan.chunks
    low = jnp.dot(even, table[:, :half], preferred_element_type=jnp.float32)
    high = jnp.dot(odd, table[:, half:], preferred_element_type=jnp.float32)
    return low + high


def two_terms(values):
    high = values.astype(jnp.bfloat16)
    low = (values - high.astype(jnp.float32)).astype(jnp.bfloat16)
    return jnp.concatenate([high, low], axis=1)


def clip_round(values):
    return jnp.clip(values, -quant_limit, quant_limit).astype(jnp.bfloat16)


def front(plan, span, mine, activations, out_grads, first_exp, flips):
    first_chunk, chunk_count = span
    group = min(8, chunk_count)
    groups = chunk_count // group
    half_rows = plan.rows // 2
    seg = plan.seg_rows
    wide = group * plan.order

    def kernel(acts_ref, grads_ref, exp_ref, flips_ref, *refs):
        outs, (grads_vmem, sems) = refs[:-2], refs[-2:]

        def copy(step):
            at = (first_chunk + step * group) * plan.order
            return pltpu.make_async_copy(
                grads_ref.at[:, pl.ds(at, wide)], grads_vmem.at[step], sems.at[step]
            )

        for step in range(groups):
            copy(step).start()
        outer_place, level, core = places()
        keeper = core if mine else 1 - core
        index = iota((half_rows, 1), 0)
        own = index & (plan.own_rows - 1)
        hop_outer = (index >> log2(plan.own_rows)) & (plan.outer - 1)
        hop_level = index >> log2(seg)
        inner_of = 2 * (level ^ hop_level) + keeper
        row_of = ((outer_place ^ hop_outer) * plan.inner + inner_of) * plan.own_rows + own
        chooser = jnp.where(
            iota((half_rows, plan.rows), 1) == jnp.broadcast_to(row_of, (half_rows, plan.rows)),
            1.0,
            0.0,
        ).astype(jnp.bfloat16)
        acts = lax.dot_general(
            chooser, acts_ref[...], (((1,), (1,)), ((), ())), preferred_element_type=jnp.float32
        ).astype(jnp.bfloat16)
        root = 1.0 / (plan.order**0.5)
        down = pick(plan, row_of, jnp.exp2(-exp_ref[...].astype(jnp.float32))) * root
        turn = jnp.concatenate([flips_ref[...], flips_ref[...]], axis=0)
        for step in range(groups):
            copy(step).wait()
            grad = jnp.dot(acts, grads_vmem[step], preferred_element_type=jnp.float32)
            stacked = jnp.concatenate(
                [grad[:, c * plan.order : (c + 1) * plan.order] for c in range(group)], axis=0
            )
            rotated = jnp.dot(two_terms(stacked), turn, preferred_element_type=jnp.float32)
            for c in range(group):
                at = first_chunk + step * group + c
                part = rotated[c * half_rows : (c + 1) * half_rows] * down[:, at : at + 1]
                part = clip_round(part)
                for hop in range(plan.levels):
                    row = (step * group + c) * seg
                    outs[hop][pl.ds(row, seg), :] = part[hop * seg : (hop + 1) * seg]

    piece = jax.ShapeDtypeStruct((chunk_count * seg, plan.order), jnp.bfloat16)
    return pl.pallas_call(
        kernel,
        out_shape=[piece] * plan.levels,
        in_specs=[
            pl.BlockSpec(memory_space=pltpu.VMEM),
            pl.BlockSpec(memory_space=pl.ANY),
            pl.BlockSpec(memory_space=pltpu.VMEM),
            pl.BlockSpec(memory_space=pltpu.VMEM),
        ],
        out_specs=[pl.BlockSpec(memory_space=pltpu.VMEM)] * plan.levels,
        scratch_shapes=[
            pltpu.VMEM((groups, plan.tokens, wide), jnp.bfloat16),
            pltpu.SemaphoreType.DMA((groups,)),
        ],
        compiler_params=vmem(16),
        name="front_mine" if mine else "front_theirs",
    )(activations, out_grads, first_exp, flips)


def join_cores(plan, span, ours, theirs):
    def kernel(*refs):
        count = plan.levels
        for hop in range(count):
            one, two, out = refs[hop], refs[count + hop], refs[2 * count + hop]
            out[...] = (one[...].astype(jnp.float32) + two[...].astype(jnp.float32)).astype(
                jnp.bfloat16
            )

    piece = jax.ShapeDtypeStruct(ours[0].shape, jnp.bfloat16)
    return pl.pallas_call(kernel, out_shape=[piece] * plan.levels, compiler_params=vmem(16), name="join_cores")(
        *ours, *theirs
    )


def requantize(plan, span, first_exp, second_exp, parts):
    first_chunk, chunk_count = span
    seg = plan.seg_rows
    group = min(16, chunk_count)
    size = group * seg

    def kernel(first_ref, second_ref, *refs):
        ins, outs = refs[: plan.levels], refs[plan.levels :]
        outer_place, level, core = places()
        index = iota((seg, 1), 0)
        own = index & (plan.own_rows - 1)
        hop = index >> log2(plan.own_rows)
        inner_of = 2 * level + core
        row_of = ((outer_place ^ hop) * plan.inner + inner_of) * plan.own_rows + own
        shift = pick(plan, row_of, jnp.exp2((first_ref[...] - second_ref[...]).astype(jnp.float32)))
        here, there = iota((size, size), 0), iota((size, size), 1)
        source = (here & (group - 1)) * seg + (here >> log2(group))
        order = jnp.where(there == source, 1.0, 0.0).astype(jnp.bfloat16)
        for step in range(chunk_count // group):
            rows = pl.ds(step * size, size)
            total = ins[0][rows, :].astype(jnp.float32)
            for other in ins[1:]:
                total = total + other[rows, :].astype(jnp.float32)
            scaled = jnp.concatenate(
                [
                    total[c * seg : (c + 1) * seg] * shift[:, at : at + 1]
                    for c, at in enumerate(range(first_chunk + step * group, first_chunk + (step + 1) * group))
                ],
                axis=0,
            )
            moved = jnp.dot(order, clip_round(scaled), preferred_element_type=jnp.float32)
            moved = moved.astype(jnp.bfloat16)
            for m in range(seg):
                out, row = outs[m // plan.own_rows], (m % plan.own_rows) * chunk_count + step * group
                out[pl.ds(row, group), :] = moved[m * group : (m + 1) * group]

    piece = jax.ShapeDtypeStruct((plan.own_rows * chunk_count, plan.order), jnp.bfloat16)
    return pl.pallas_call(kernel, out_shape=[piece] * plan.outer, compiler_params=vmem(12), name="requantize")(
        first_exp, second_exp, *parts
    )


def owner(plan, span, second_exp, third_exp, flips_one, flips_two, momentum, parts):
    first_chunk, chunk_count = span
    own_rows, order = plan.own_rows, plan.order
    devices = plan.outer * plan.inner

    def kernel(second_ref, third_ref, one_ref, two_ref, momentum_ref, *refs):
        ins, (moment_out, update_out) = refs[: plan.outer], refs[plan.outer :]
        outer_place, level, core = places()
        first_row = (outer_place * plan.inner + 2 * level + core) * own_rows
        row_of = first_row + iota((own_rows, 1), 0)
        diagonal = iota((chunk_count, chunk_count), 0) == iota((chunk_count, chunk_count), 1)

        def column(table):
            chosen = pick(plan, row_of, table)[:, first_chunk : first_chunk + chunk_count]
            return jnp.concatenate(
                [
                    jnp.sum(jnp.where(diagonal, chosen[k : k + 1], 0.0), axis=1, keepdims=True)
                    for k in range(own_rows)
                ],
                axis=0,
            )

        second = second_ref[...].astype(jnp.float32)
        third = third_ref[...].astype(jnp.float32)
        up, third_down, third_up = (column(jnp.exp2(e)) for e in (second, -third, third))
        root = 1.0 / (order**0.5)
        total = ins[0][...].astype(jnp.float32)
        for other in ins[1:]:
            total = total + other[...].astype(jnp.float32)
        one, two = one_ref[...], two_ref[...]
        back = lax.dot_general(
            two_terms(total * up),
            jnp.concatenate([one, one], axis=1),
            (((1,), (1,)), ((), ())),
            preferred_element_type=jnp.float32,
        )
        before = jnp.concatenate(
            [
                momentum_ref[pl.ds(k * plan.chunks + first_chunk, chunk_count), :]
                for k in range(own_rows)
            ],
            axis=0,
        )
        moment = momentum_decay * before + back * (root / devices)
        moment_out[...] = moment
        turned = jnp.dot(
            two_terms(-step_size * moment),
            jnp.concatenate([two, two], axis=0),
            preferred_element_type=jnp.float32,
        )
        quant = clip_round(turned * (third_down * root))
        restored = lax.dot_general(
            quant, two, (((1,), (1,)), ((), ())), preferred_element_type=jnp.float32
        )
        update_out[...] = (restored * (third_up * root)).astype(jnp.bfloat16)

    shape = (own_rows * chunk_count, order)
    return pl.pallas_call(
        kernel,
        out_shape=[
            jax.ShapeDtypeStruct(shape, jnp.float32),
            jax.ShapeDtypeStruct(shape, jnp.bfloat16),
        ],
        compiler_params=vmem(8),
        name="owner",
    )(second_exp, third_exp, flips_one, flips_two, momentum, *parts)


def half_slab(plan, span, parts):
    first_chunk, chunk_count = span
    own_rows, rows = plan.own_rows, plan.slab_rows
    group = min(16, chunk_count)
    size = group * rows

    def kernel(*refs):
        ins, out = refs[:-1], refs[-1]
        outer_place, level, core = places()
        here, there = iota((size, size), 0), iota((size, size), 1)
        row = here & (rows - 1)
        hop = (row >> log2(own_rows)) ^ level
        source = (hop * own_rows + (row & (own_rows - 1))) * group + (here >> log2(rows))
        order = jnp.where(there == source, 1.0, 0.0).astype(jnp.bfloat16)
        for step in range(chunk_count // group):
            block = jnp.concatenate(
                [
                    part[pl.ds(k * chunk_count + step * group, group), :]
                    for part in ins
                    for k in range(own_rows)
                ],
                axis=0,
            )
            moved = jnp.dot(order, block, preferred_element_type=jnp.float32).astype(jnp.bfloat16)
            for c in range(group):
                at = (step * group + c) * plan.order
                out[:, pl.ds(at, plan.order)] = moved[c * rows : (c + 1) * rows]

    shape = jax.ShapeDtypeStruct((rows, chunk_count * plan.order), jnp.bfloat16)
    return pl.pallas_call(kernel, out_shape=shape, compiler_params=vmem(8), name="half_slab")(*parts)


def place_slabs(plan, ours, theirs):
    spans = plan.spans

    def kernel(*refs):
        (out, sems), ins = refs[-2:], refs[:-2]
        outer_place, level, core = places()
        copies = []
        for n, (first_chunk, chunk_count) in enumerate(spans):
            for side in range(2):
                keeper = core if side == 0 else 1 - core
                for hop in range(plan.outer):
                    at = (n * 2 + side) * plan.outer + hop
                    row = ((outer_place ^ hop) * 2 + keeper) * plan.slab_rows
                    copies.append(
                        pltpu.make_async_copy(
                            ins[at],
                            out.at[
                                pl.ds(row, plan.slab_rows),
                                pl.ds(first_chunk * plan.order, chunk_count * plan.order),
                            ],
                            sems.at[at],
                        )
                    )
        for copy in copies:
            copy.start()
        for copy in copies:
            copy.wait()

    flat = [piece for n in range(len(spans)) for side in (ours[n], theirs[n]) for piece in side]
    return pl.pallas_call(
        kernel,
        out_shape=jax.ShapeDtypeStruct((plan.rows, plan.width), jnp.bfloat16),
        in_specs=[pl.BlockSpec(memory_space=pl.ANY)] * len(flat),
        out_specs=pl.BlockSpec(memory_space=pl.ANY),
        scratch_shapes=[pltpu.SemaphoreType.DMA((len(flat),))],
        compiler_params=vmem(8),
        name="place_slabs",
    )(*flat)


def send(plan, value, target_of):
    pairs = []
    for o in range(plan.outer):
        for z in range(plan.levels):
            for c in range(2):
                to, tz, tc = target_of(o, z, c)
                pairs.append((o * plan.inner + 2 * z + c, to * plan.inner + 2 * tz + tc))
    return lax.ppermute(value, ("outer", "inner"), pairs)


def swap_cores(plan, value):
    return send(plan, value, lambda o, z, c: (o, z, 1 - c))


def over_levels(plan, value, hop):
    return send(plan, value, lambda o, z, c: (o, z ^ hop, c))


def over_outer(plan, value, hop):
    return send(plan, value, lambda o, z, c: (o ^ hop, z, c))


def to_band(plan, value, hop):
    band = plan.levels // 2
    return send(
        plan, value, lambda o, z, c: (o, (2 * (z & (band - 1)) + c) ^ hop, z // band)
    )


def stream(plan, span, tables, activations, out_grads, momentum):
    first_exp, second_exp, third_exp, flips_one, flips_two = tables
    theirs = front(plan, span, False, activations, out_grads, first_exp, flips_one)
    theirs = [swap_cores(plan, piece) for piece in theirs]
    ours = front(plan, span, True, activations, out_grads, first_exp, flips_one)
    joined = join_cores(plan, span, ours, theirs)
    parts = [joined[0]] + [over_levels(plan, joined[hop], hop) for hop in range(1, plan.levels)]
    parts = requantize(plan, span, first_exp, second_exp, parts)
    parts = [parts[0]] + [over_outer(plan, parts[hop], hop) for hop in range(1, plan.outer)]
    moment, update = owner(plan, span, second_exp, third_exp, flips_one, flips_two, momentum, parts)
    band = [to_band(plan, update, hop) for hop in range(plan.levels)]
    slab = half_slab(plan, span, band)
    ours = [slab] + [over_outer(plan, slab, hop) for hop in range(1, plan.outer)]
    theirs = [swap_cores(plan, piece) for piece in ours]
    return moment, ours, theirs


def on_device(activations, out_grads, momentum, first_exp, second_exp, third_exp, signs):
    plan = Plan(activations, out_grads, signs, lax.axis_size("outer"), lax.axis_size("inner"))
    if not plan.fits():
        return general(activations, out_grads, momentum, first_exp, second_exp, third_exp, signs)
    plan.spans = split_chunks(plan.chunks)
    flips = 1.0 - 2.0 * signs.astype(jnp.float32)
    turns = (flips[:, :, None] * hadamard_matrix(plan.order)[None]).astype(jnp.bfloat16)
    exps = [e.reshape(-1, plan.order) for e in (first_exp, second_exp, third_exp)]
    tables = (*exps, turns[0], turns[1])
    done = [stream(plan, span, tables, activations, out_grads, momentum) for span in plan.spans]
    moments = [d[0].reshape(plan.own_rows, -1, plan.order) for d in done]
    new_momentum = jnp.concatenate(moments, axis=1).reshape(momentum.shape)
    update = place_slabs(plan, [d[1] for d in done], [d[2] for d in done])
    return (new_momentum, update)


def split_chunks(chunks):
    return [(0, chunks)]


def solution(mesh):
    in_specs = (
        P(("outer", "inner"), None),
        P(("outer", "inner"), None),
        P(("outer", "inner"), None),
        P(),
        P(),
        P(),
        P(),
    )
    out_specs = (P(("outer", "inner"), None), P())
    return jax.shard_map(
        on_device, mesh=mesh, in_specs=in_specs, out_specs=out_specs, check_vma=False
    )
```

```python
import jax
import jax.numpy as jnp
from jax import lax
from jax.experimental import pallas as pl
from jax.experimental.pallas import tpu as pltpu
from jax.sharding import PartitionSpec as P


quant_limit = 127.0
momentum_decay = 0.9
step_size = 0.5


def hadamard_matrix(order):
    position = jnp.arange(order, dtype=jnp.int32)
    common = jnp.bitwise_and(position[:, None], position[None, :])
    parity = jnp.zeros((order, order), jnp.int32)
    for shift_by in range(order.bit_length() - 1):
        parity = parity + jnp.bitwise_and(jnp.right_shift(common, shift_by), 1)
    return 1.0 - 2.0 * jnp.bitwise_and(parity, 1).astype(jnp.float32)


def rotation(sign_bits):
    order = sign_bits.shape[0]
    flips = 1.0 - 2.0 * sign_bits.astype(jnp.float32)
    return flips[:, None] * hadamard_matrix(order) / jnp.sqrt(jnp.float32(order))


def collect(pieces):
    grouped = lax.all_gather(pieces[None], "outer", axis=0, tiled=True)
    spread = lax.all_gather(grouped, "inner", axis=1, tiled=True)
    return spread.reshape(-1, pieces.shape[1])


def general(activations, out_grads, momentum, first_exp, second_exp, third_exp, signs):
    high = lax.Precision.HIGHEST
    outer_count = lax.axis_size("outer")
    inner_count = lax.axis_size("inner")
    outer_place = lax.axis_index("outer")
    inner_place = lax.axis_index("inner")
    device_count = outer_count * inner_count
    first_rot = rotation(signs[0])
    second_rot = rotation(signs[1])
    grad = lax.dot_general(
        activations, out_grads, (((0,), (0,)), ((), ())), preferred_element_type=jnp.float32
    )
    slab_shape = grad.shape
    order = first_rot.shape[0]
    count_blocks = grad.size // order
    shard_rows = count_blocks // device_count
    rotated = jnp.dot(grad.reshape(count_blocks, order), first_rot, precision=high)
    first_down = jnp.exp2(-first_exp.astype(jnp.float32))[:, None]
    quant_first = jnp.clip(rotated * first_down, -quant_limit, quant_limit).astype(jnp.bfloat16)
    grouped = quant_first.astype(jnp.float32).reshape(outer_count, inner_count * shard_rows, order)
    inner_total = lax.psum_scatter(
        grouped.astype(jnp.bfloat16), "inner", scatter_dimension=1, tiled=True
    ).astype(jnp.float32)
    first_grid = first_exp.reshape(outer_count, inner_count, shard_rows)
    second_grid = second_exp.reshape(outer_count, inner_count, shard_rows)
    third_grid = third_exp.reshape(outer_count, inner_count, shard_rows)
    first_here = lax.dynamic_index_in_dim(first_grid, inner_place, 1, keepdims=False)
    second_here = lax.dynamic_index_in_dim(second_grid, inner_place, 1, keepdims=False)
    shift_scale = jnp.exp2((first_here - second_here).astype(jnp.float32))[:, :, None]
    requant = jnp.clip(inner_total * shift_scale, -quant_limit, quant_limit).astype(jnp.bfloat16)
    total = lax.psum_scatter(
        requant.astype(jnp.float32).astype(jnp.bfloat16), "outer", scatter_dimension=0, tiled=True
    ).astype(jnp.float32)[0]
    second_mine = lax.dynamic_index_in_dim(second_here, outer_place, 0, keepdims=False)
    second_up = jnp.exp2(second_mine.astype(jnp.float32))[:, None]
    mean_grad = jnp.dot(total * second_up, first_rot.T, precision=high) / device_count
    new_momentum = momentum_decay * momentum + mean_grad
    third_row = lax.dynamic_index_in_dim(third_grid, outer_place, 0, keepdims=False)
    third_mine = lax.dynamic_index_in_dim(third_row, inner_place, 0, keepdims=False)
    rotated_step = jnp.dot(-step_size * new_momentum, second_rot, precision=high)
    third_down = jnp.exp2(-third_mine.astype(jnp.float32))[:, None]
    quant_third = jnp.clip(rotated_step * third_down, -quant_limit, quant_limit).astype(
        jnp.bfloat16
    )
    third_up = jnp.exp2(third_mine.astype(jnp.float32))[:, None]
    restored = jnp.dot(quant_third.astype(jnp.float32) * third_up, second_rot.T, precision=high)
    update = collect(restored.astype(jnp.bfloat16)).reshape(slab_shape)
    return (new_momentum, update)


def vmem(mebibytes):
    return pltpu.CompilerParams(vmem_limit_bytes=mebibytes * 1024 * 1024)


def log2(count):
    return count.bit_length() - 1


def tile(count, most):
    return min(count & -count, most)


def power_of_two(count):
    return count > 0 and count & (count - 1) == 0


class Plan:
    def __init__(self, activations, out_grads, signs, outer, inner):
        self.outer, self.inner = outer, inner
        self.levels = inner // 2
        self.tokens, self.rows = activations.shape
        self.order = signs.shape[1]
        self.width = out_grads.shape[1]
        self.chunks = self.width // self.order
        self.own_rows = self.rows // (outer * inner)
        self.seg_rows = outer * self.own_rows
        self.slab_rows = self.levels * self.own_rows

    def fits(self):
        return (
            all(power_of_two(n) for n in (self.outer, self.inner, self.rows, self.chunks))
            and self.levels == 4
            and self.own_rows * self.outer * self.inner == self.rows
            and self.seg_rows == 16
            and self.slab_rows == 16
            and self.order == 128
            and 2 * self.chunks == self.order
        )


def places():
    outer_place = lax.axis_index("outer")
    inner_place = lax.axis_index("inner")
    return outer_place, inner_place >> 1, inner_place & 1


def iota(shape, axis):
    return lax.broadcasted_iota(jnp.int32, shape, axis)


def pick(plan, row_of, scale):
    count = row_of.shape[0]
    lines = scale.shape[0]
    line = iota((count, lines), 1)
    row_of = jnp.broadcast_to(row_of, (count, lines))
    even = jnp.where(row_of == 2 * line, 1.0, 0.0).astype(jnp.bfloat16)
    odd = jnp.where(row_of == 2 * line + 1, 1.0, 0.0).astype(jnp.bfloat16)
    table = scale.astype(jnp.bfloat16)
    half = plan.chunks
    low = jnp.dot(even, table[:, :half], preferred_element_type=jnp.float32)
    high = jnp.dot(odd, table[:, half:], preferred_element_type=jnp.float32)
    return low + high


def two_terms(values):
    high = values.astype(jnp.bfloat16)
    low = (values - high.astype(jnp.float32)).astype(jnp.bfloat16)
    return jnp.concatenate([high, low], axis=1)


def clip_round(values):
    return jnp.clip(values, -quant_limit, quant_limit).astype(jnp.bfloat16)


def turn_matrix(order):
    bits = iota((order, order), 0) & iota((order, order), 1)
    for shift_by in (4, 2, 1):
        bits = bits ^ (bits >> shift_by)
    return (1 - 2 * (bits & 1)).astype(jnp.float32).astype(jnp.bfloat16)


def front(plan, span, mine, activations, out_grads, first_exp, signs):
    first_chunk, chunk_count = span
    group = tile(chunk_count, 8)
    groups = chunk_count // group
    half_rows = plan.rows // 2
    seg = plan.seg_rows
    wide = group * plan.order

    def kernel(acts_hbm, grads_hbm, exp_hbm, signs_hbm, *refs):
        out, (acts_ref, grads_ref, exp_ref, signs_ref, sems) = refs[0], refs[1:]
        copies = [
            pltpu.make_async_copy(signs_hbm, signs_ref, sems.at[0]),
            pltpu.make_async_copy(acts_hbm, acts_ref, sems.at[1]),
            pltpu.make_async_copy(exp_hbm, exp_ref, sems.at[2]),
        ]
        for step in range(groups):
            at = (first_chunk + step * group) * plan.order
            copies.append(
                pltpu.make_async_copy(
                    grads_hbm.at[:, pl.ds(at, wide)], grads_ref.at[step], sems.at[3 + step]
                )
            )
        for copy in copies:
            copy.start()
        outer_place, level, core = places()
        keeper = core if mine else 1 - core
        index = iota((half_rows, 1), 0)
        own = index & (plan.own_rows - 1)
        hop_outer = (index >> log2(plan.own_rows)) & (plan.outer - 1)
        hop_level = index >> log2(seg)
        inner_of = 2 * (level ^ hop_level) + keeper
        row_of = ((outer_place ^ hop_outer) * plan.inner + inner_of) * plan.own_rows + own
        chooser = jnp.where(
            iota((half_rows, plan.rows), 1) == jnp.broadcast_to(row_of, (half_rows, plan.rows)),
            1.0,
            0.0,
        ).astype(jnp.bfloat16)
        root = 1.0 / (plan.order**0.5)
        square = (plan.order, plan.order)
        hadamard = turn_matrix(plan.order)
        for copy in copies:
            copy.wait()
        flips = 1.0 - 2.0 * signs_ref[0:1, :].astype(jnp.float32)
        diagonal = jnp.where(iota(square, 0) == iota(square, 1), flips, 0.0).astype(jnp.bfloat16)
        turn = jnp.dot(diagonal, hadamard, preferred_element_type=jnp.float32).astype(jnp.bfloat16)
        turn = jnp.concatenate([turn, turn], axis=0)
        acts = lax.dot_general(
            chooser, acts_ref[...], (((1,), (1,)), ((), ())), preferred_element_type=jnp.float32
        ).astype(jnp.bfloat16)
        down = pick(plan, row_of, jnp.exp2(-exp_ref[...].astype(jnp.float32))) * root
        for step in range(groups):
            grad = jnp.dot(acts, grads_ref[step], preferred_element_type=jnp.float32)
            stacked = jnp.concatenate(
                [grad[:, c * plan.order : (c + 1) * plan.order] for c in range(group)], axis=0
            )
            rotated = jnp.dot(two_terms(stacked), turn, preferred_element_type=jnp.float32)
            for c in range(group):
                at = first_chunk + step * group + c
                part = rotated[c * half_rows : (c + 1) * half_rows] * down[:, at : at + 1]
                part = clip_round(part)
                for hop in range(plan.levels):
                    row = (hop * chunk_count + step * group + c) * seg
                    out[pl.ds(row, seg), :] = part[hop * seg : (hop + 1) * seg]

    return pl.pallas_call(
        kernel,
        out_shape=jax.ShapeDtypeStruct(
            (plan.levels * chunk_count * seg, plan.order), jnp.bfloat16
        ),
        in_specs=[pl.BlockSpec(memory_space=pltpu.HBM)] * 4,
        out_specs=pl.BlockSpec(memory_space=pltpu.VMEM),
        scratch_shapes=[
            pltpu.VMEM(activations.shape, jnp.bfloat16),
            pltpu.VMEM((groups, plan.tokens, wide), jnp.bfloat16),
            pltpu.VMEM(first_exp.shape, jnp.int32),
            pltpu.VMEM(signs.shape, jnp.int32),
            pltpu.SemaphoreType.DMA((groups + 3,)),
        ],
        compiler_params=vmem(16 if mine or first_chunk else 60),
        name="front_mine" if mine else "front_theirs",
    )(activations, out_grads, first_exp, signs)


def join_cores(plan, ours, theirs):
    rows = ours.shape[0] // plan.levels

    def kernel(one, two, *outs):
        for hop, out in enumerate(outs):
            at = pl.ds(hop * rows, rows)
            total = one[at, :].astype(jnp.float32) + two[at, :].astype(jnp.float32)
            out[...] = total.astype(jnp.bfloat16)

    piece = jax.ShapeDtypeStruct((rows, ours.shape[1]), jnp.bfloat16)
    return pl.pallas_call(
        kernel, out_shape=[piece] * plan.levels, compiler_params=vmem(16), name="join_cores"
    )(ours, theirs)


def requantize(plan, spans, first_exp, second_exp, parts):
    first_chunk, chunk_count = whole_span(spans)
    seg = plan.seg_rows
    levels = plan.levels

    def kernel(first_ref, second_ref, *refs):
        ins, outs = refs[: levels * len(spans)], refs[levels * len(spans) :]
        outer_place, level, core = places()
        index = iota((seg, 1), 0)
        own = index & (plan.own_rows - 1)
        hop = index >> log2(plan.own_rows)
        inner_of = 2 * level + core
        row_of = ((outer_place ^ hop) * plan.inner + inner_of) * plan.own_rows + own
        shift = pick(plan, row_of, jnp.exp2((first_ref[...] - second_ref[...]).astype(jnp.float32)))
        for n, (span_chunk, span_count) in enumerate(spans):
            group = tile(span_count, 16)
            size = group * seg
            here, there = iota((size, size), 0), iota((size, size), 1)
            source = (here & (group - 1)) * seg + (here >> log2(group))
            order = jnp.where(there == source, 1.0, 0.0).astype(jnp.bfloat16)
            for step in range(span_count // group):
                rows = pl.ds(step * size, size)
                total = ins[n * levels][rows, :].astype(jnp.float32)
                for other in ins[n * levels + 1 : (n + 1) * levels]:
                    total = total + other[rows, :].astype(jnp.float32)
                start = span_chunk + step * group
                scaled = jnp.concatenate(
                    [
                        total[c * seg : (c + 1) * seg] * shift[:, start + c : start + c + 1]
                        for c in range(group)
                    ],
                    axis=0,
                )
                moved = jnp.dot(order, clip_round(scaled), preferred_element_type=jnp.float32)
                moved = moved.astype(jnp.bfloat16)
                for m in range(seg):
                    row = (m % plan.own_rows) * chunk_count + start - first_chunk
                    outs[m // plan.own_rows][pl.ds(row, group), :] = moved[
                        m * group : (m + 1) * group
                    ]

    piece = jax.ShapeDtypeStruct((plan.own_rows * chunk_count, plan.order), jnp.bfloat16)
    return pl.pallas_call(
        kernel, out_shape=[piece] * plan.outer, compiler_params=vmem(12), name="requantize"
    )(first_exp, second_exp, *[piece for span_parts in parts for piece in span_parts])


def whole_span(spans):
    return (spans[0][0], sum(count for start, count in spans))


def owner(plan, span, second_exp, third_exp, signs, momentum, parts):
    first_chunk, chunk_count = span
    own_rows, order = plan.own_rows, plan.order
    devices = plan.outer * plan.inner

    def kernel(second_ref, third_ref, signs_ref, momentum_ref, *refs):
        ins, (moment_out, update_out) = refs[: plan.outer], refs[plan.outer :]
        outer_place, level, core = places()
        first_row = (outer_place * plan.inner + 2 * level + core) * own_rows
        row_of = first_row + iota((own_rows, 1), 0)
        diagonal = iota((chunk_count, chunk_count), 0) == iota((chunk_count, chunk_count), 1)

        def column(table):
            chosen = pick(plan, row_of, table)[:, first_chunk : first_chunk + chunk_count]
            return jnp.concatenate(
                [
                    jnp.sum(jnp.where(diagonal, chosen[k : k + 1], 0.0), axis=1, keepdims=True)
                    for k in range(own_rows)
                ],
                axis=0,
            )

        second = second_ref[...].astype(jnp.float32)
        third = third_ref[...].astype(jnp.float32)
        up, third_down, third_up = (column(jnp.exp2(e)) for e in (second, -third, third))
        root = 1.0 / (order**0.5)
        total = ins[0][...].astype(jnp.float32)
        for other in ins[1:]:
            total = total + other[...].astype(jnp.float32)
        flips = 1.0 - 2.0 * signs_ref[...].astype(jnp.float32)
        one, two = flips[0:1, :], flips[1:2, :]
        turn = turn_matrix(order)
        twice = jnp.concatenate([turn, turn], axis=0)
        back = jnp.dot(two_terms(total * up), twice, preferred_element_type=jnp.float32)
        before = jnp.concatenate(
            [
                momentum_ref[pl.ds(k * plan.chunks + first_chunk, chunk_count), :]
                for k in range(own_rows)
            ],
            axis=0,
        )
        moment = momentum_decay * before + back * (one * (root / devices))
        moment_out[...] = moment
        turned = jnp.dot(
            two_terms(moment * (-step_size * two)), twice, preferred_element_type=jnp.float32
        )
        quant = clip_round(turned * (third_down * root))
        restored = jnp.dot(quant, turn, preferred_element_type=jnp.float32)
        update_out[...] = (restored * (third_up * root) * two).astype(jnp.bfloat16)

    shape = (own_rows * chunk_count, order)
    return pl.pallas_call(
        kernel,
        out_shape=[
            jax.ShapeDtypeStruct(shape, jnp.float32),
            jax.ShapeDtypeStruct(shape, jnp.bfloat16),
        ],
        compiler_params=vmem(8),
        name="owner",
    )(second_exp, third_exp, signs, momentum, *parts)


def band_of(level, core):
    return core ^ (level >> 1)


def half_slab(plan, span, pair, near, far):
    _, chunk_count = span
    own_rows, rows = plan.own_rows, plan.slab_rows
    group = tile(chunk_count, 16)
    size = group * rows

    def kernel(pair_ref, near_ref, far_ref, out):
        _, level, core = places()
        here, there = iota((size, size), 0), iota((size, size), 1)
        row = here & (rows - 1)
        device = row >> log2(own_rows)
        side = ((device >> 1) ^ level) & 1
        part = 2 * side + ((device ^ core) & 1)
        source = (part * own_rows + (row & (own_rows - 1))) * group + (here >> log2(rows))
        order = jnp.where(there == source, 1.0, 0.0).astype(jnp.bfloat16)
        lower = core == 0
        for step in range(chunk_count // group):
            blocks = []
            for one, two in ((pair_ref, near_ref), (near_ref, far_ref)):
                for k in range(2 * own_rows):
                    at = pl.ds(k * chunk_count + step * group, group)
                    blocks.append(jnp.where(lower, one[at, :], two[at, :]))
            block = jnp.concatenate(blocks, axis=0)
            moved = jnp.dot(order, block, preferred_element_type=jnp.float32).astype(jnp.bfloat16)
            for c in range(group):
                at = (step * group + c) * plan.order
                out[:, pl.ds(at, plan.order)] = moved[c * rows : (c + 1) * rows]

    shape = jax.ShapeDtypeStruct((rows, chunk_count * plan.order), jnp.bfloat16)
    return pl.pallas_call(
        kernel, out_shape=shape, compiler_params=vmem(8), name="half_slab"
    )(pair, near, far)


def place_slabs(plan, ours, theirs):
    spans = plan.spans

    def kernel(*refs):
        (out, sems), ins = refs[-2:], refs[:-2]
        outer_place, level, core = places()
        copies = []
        for n, (first_chunk, chunk_count) in enumerate(spans):
            for side in range(2):
                band = band_of(level, core) if side == 0 else 1 - band_of(level, core)
                for hop in range(plan.outer):
                    at = (n * 2 + side) * plan.outer + hop
                    row = ((outer_place ^ hop) * 2 + band) * plan.slab_rows
                    copies.append(
                        pltpu.make_async_copy(
                            ins[at],
                            out.at[
                                pl.ds(row, plan.slab_rows),
                                pl.ds(first_chunk * plan.order, chunk_count * plan.order),
                            ],
                            sems.at[at],
                        )
                    )
        for copy in copies:
            copy.start()
        for copy in copies:
            copy.wait()

    flat = [piece for n in range(len(spans)) for side in (ours[n], theirs[n]) for piece in side]
    return pl.pallas_call(
        kernel,
        out_shape=jax.ShapeDtypeStruct((plan.rows, plan.width), jnp.bfloat16),
        in_specs=[pl.BlockSpec(memory_space=pl.ANY)] * len(flat),
        out_specs=pl.BlockSpec(memory_space=pl.ANY),
        scratch_shapes=[pltpu.SemaphoreType.DMA((len(flat),))],
        compiler_params=vmem(8),
        name="place_slabs",
    )(*flat)


def send(plan, value, target_of):
    pairs = []
    for o in range(plan.outer):
        for z in range(plan.levels):
            for c in range(2):
                target = target_of(o, z, c)
                if target is not None:
                    to, tz, tc = target
                    pairs.append((o * plan.inner + 2 * z + c, to * plan.inner + 2 * tz + tc))
    return lax.ppermute(value, ("outer", "inner"), pairs)


def swap_cores(plan, value):
    return send(plan, value, lambda o, z, c: (o, z, 1 - c))


def over_levels(plan, value, hop):
    return send(plan, value, lambda o, z, c: (o, z ^ hop, c))


def over_outer(plan, value, hop):
    return send(plan, value, lambda o, z, c: (o ^ hop, z, c))


def to_near(plan, value):
    return send(plan, value, lambda o, z, c: (o, z ^ (2 if c else 1), c))


def to_far(plan, value):
    return send(plan, value, lambda o, z, c: (o, z ^ 3, c) if c else None)


def stream_front(plan, span, activations, out_grads, first_exp, signs):
    theirs = front(plan, span, False, activations, out_grads, first_exp, signs)
    theirs = swap_cores(plan, theirs)
    ours = front(plan, span, True, activations, out_grads, first_exp, signs)
    joined = join_cores(plan, ours, theirs)
    parts = [joined[0]]
    for hop in range(1, plan.levels):
        parts.append(over_levels(plan, joined[hop], hop))
    return parts


def stream_back(plan, spans, tables, momentum, parts):
    first_exp, second_exp, third_exp, signs = tables
    span = whole_span(spans)
    parts = requantize(plan, spans, first_exp, second_exp, parts)
    pieces = [parts[0]]
    for hop in range(1, plan.outer):
        pieces.append(over_outer(plan, parts[hop], hop))
    moment, update = owner(plan, span, second_exp, third_exp, signs, momentum, pieces)
    pair = jnp.concatenate([update, swap_cores(plan, update)], axis=0)
    near = to_near(plan, pair)
    far = to_far(plan, pair)
    slab = half_slab(plan, span, pair, near, far)
    ours = [slab]
    for hop in range(1, plan.outer):
        ours.append(over_outer(plan, slab, hop))
    theirs = []
    for hop in range(plan.outer):
        theirs.append(swap_cores(plan, ours[hop]))
    return moment, ours, theirs


def on_device(activations, out_grads, momentum, first_exp, second_exp, third_exp, signs):
    plan = Plan(activations, out_grads, signs, lax.axis_size("outer"), lax.axis_size("inner"))
    if not plan.fits():
        return general(activations, out_grads, momentum, first_exp, second_exp, third_exp, signs)
    exps = [e.reshape(-1, plan.order) for e in (first_exp, second_exp, third_exp)]
    groups = split_chunks(plan.chunks)
    plan.spans = [whole_span(spans) for spans in groups]
    fronts = {}
    for spans in groups:
        for span in spans:
            fronts[span] = stream_front(plan, span, activations, out_grads, exps[0], signs)
    done = [
        stream_back(plan, spans, (*exps, signs), momentum, [fronts[span] for span in spans])
        for spans in groups
    ]
    moments = [d[0].reshape(plan.own_rows, -1, plan.order) for d in done]
    new_momentum = jnp.concatenate(moments, axis=1).reshape(momentum.shape)
    update = place_slabs(plan, [d[1] for d in done], [d[2] for d in done])
    return (new_momentum, update)


def split_chunks(chunks):
    half = chunks // 2
    return [[(0, half), (half, chunks - half)]]


def solution(mesh):
    in_specs = (
        P(("outer", "inner"), None),
        P(("outer", "inner"), None),
        P(("outer", "inner"), None),
        P(),
        P(),
        P(),
        P(),
    )
    out_specs = (P(("outer", "inner"), None), P())
    return jax.shard_map(
        on_device, mesh=mesh, in_specs=in_specs, out_specs=out_specs, check_vma=False
    )
```

```python
import jax
import jax.numpy as jnp
from jax import lax
from jax.experimental import pallas as pl
from jax.experimental.pallas import tpu as pltpu
from jax.sharding import PartitionSpec as P


quant_limit = 127.0
momentum_decay = 0.9
step_size = 0.5


def hadamard_matrix(order):
    position = jnp.arange(order, dtype=jnp.int32)
    common = jnp.bitwise_and(position[:, None], position[None, :])
    parity = jnp.zeros((order, order), jnp.int32)
    for shift_by in range(order.bit_length() - 1):
        parity = parity + jnp.bitwise_and(jnp.right_shift(common, shift_by), 1)
    return 1.0 - 2.0 * jnp.bitwise_and(parity, 1).astype(jnp.float32)


def rotation(sign_bits):
    order = sign_bits.shape[0]
    flips = 1.0 - 2.0 * sign_bits.astype(jnp.float32)
    return flips[:, None] * hadamard_matrix(order) / jnp.sqrt(jnp.float32(order))


def collect(pieces):
    grouped = lax.all_gather(pieces[None], "outer", axis=0, tiled=True)
    spread = lax.all_gather(grouped, "inner", axis=1, tiled=True)
    return spread.reshape(-1, pieces.shape[1])


def general(activations, out_grads, momentum, first_exp, second_exp, third_exp, signs):
    high = lax.Precision.HIGHEST
    outer_count = lax.axis_size("outer")
    inner_count = lax.axis_size("inner")
    outer_place = lax.axis_index("outer")
    inner_place = lax.axis_index("inner")
    device_count = outer_count * inner_count
    first_rot = rotation(signs[0])
    second_rot = rotation(signs[1])
    grad = lax.dot_general(
        activations, out_grads, (((0,), (0,)), ((), ())), preferred_element_type=jnp.float32
    )
    slab_shape = grad.shape
    order = first_rot.shape[0]
    count_blocks = grad.size // order
    shard_rows = count_blocks // device_count
    rotated = jnp.dot(grad.reshape(count_blocks, order), first_rot, precision=high)
    first_down = jnp.exp2(-first_exp.astype(jnp.float32))[:, None]
    quant_first = jnp.clip(rotated * first_down, -quant_limit, quant_limit).astype(jnp.bfloat16)
    grouped = quant_first.astype(jnp.float32).reshape(outer_count, inner_count * shard_rows, order)
    inner_total = lax.psum_scatter(
        grouped.astype(jnp.bfloat16), "inner", scatter_dimension=1, tiled=True
    ).astype(jnp.float32)
    first_grid = first_exp.reshape(outer_count, inner_count, shard_rows)
    second_grid = second_exp.reshape(outer_count, inner_count, shard_rows)
    third_grid = third_exp.reshape(outer_count, inner_count, shard_rows)
    first_here = lax.dynamic_index_in_dim(first_grid, inner_place, 1, keepdims=False)
    second_here = lax.dynamic_index_in_dim(second_grid, inner_place, 1, keepdims=False)
    shift_scale = jnp.exp2((first_here - second_here).astype(jnp.float32))[:, :, None]
    requant = jnp.clip(inner_total * shift_scale, -quant_limit, quant_limit).astype(jnp.bfloat16)
    total = lax.psum_scatter(
        requant.astype(jnp.float32).astype(jnp.bfloat16), "outer", scatter_dimension=0, tiled=True
    ).astype(jnp.float32)[0]
    second_mine = lax.dynamic_index_in_dim(second_here, outer_place, 0, keepdims=False)
    second_up = jnp.exp2(second_mine.astype(jnp.float32))[:, None]
    mean_grad = jnp.dot(total * second_up, first_rot.T, precision=high) / device_count
    new_momentum = momentum_decay * momentum + mean_grad
    third_row = lax.dynamic_index_in_dim(third_grid, outer_place, 0, keepdims=False)
    third_mine = lax.dynamic_index_in_dim(third_row, inner_place, 0, keepdims=False)
    rotated_step = jnp.dot(-step_size * new_momentum, second_rot, precision=high)
    third_down = jnp.exp2(-third_mine.astype(jnp.float32))[:, None]
    quant_third = jnp.clip(rotated_step * third_down, -quant_limit, quant_limit).astype(
        jnp.bfloat16
    )
    third_up = jnp.exp2(third_mine.astype(jnp.float32))[:, None]
    restored = jnp.dot(quant_third.astype(jnp.float32) * third_up, second_rot.T, precision=high)
    update = collect(restored.astype(jnp.bfloat16)).reshape(slab_shape)
    return (new_momentum, update)


def vmem(mebibytes):
    return pltpu.CompilerParams(vmem_limit_bytes=mebibytes * 1024 * 1024)


def log2(count):
    return count.bit_length() - 1


def tile(count, most):
    return min(count & -count, most)


def power_of_two(count):
    return count > 0 and count & (count - 1) == 0


class Plan:
    def __init__(self, activations, out_grads, signs, outer, inner):
        self.outer, self.inner = outer, inner
        self.levels = inner // 2
        self.tokens, self.rows = activations.shape
        self.order = signs.shape[1]
        self.width = out_grads.shape[1]
        self.chunks = self.width // self.order
        self.own_rows = self.rows // (outer * inner)
        self.seg_rows = outer * self.own_rows
        self.slab_rows = self.levels * self.own_rows

    def fits(self):
        return (
            all(power_of_two(n) for n in (self.outer, self.inner, self.rows, self.chunks))
            and self.levels == 4
            and self.own_rows * self.outer * self.inner == self.rows
            and self.seg_rows == 16
            and self.slab_rows == 16
            and self.outer == 4
            and self.order == 128
            and 2 * self.chunks == self.order
        )


def places():
    outer_place = lax.axis_index("outer")
    inner_place = lax.axis_index("inner")
    return outer_place, inner_place >> 1, inner_place & 1


def iota(shape, axis):
    return lax.broadcasted_iota(jnp.int32, shape, axis)


def pick(plan, row_of, scale):
    count = row_of.shape[0]
    lines = scale.shape[0]
    line = iota((count, lines), 1)
    row_of = jnp.broadcast_to(row_of, (count, lines))
    even = jnp.where(row_of == 2 * line, 1.0, 0.0).astype(jnp.bfloat16)
    odd = jnp.where(row_of == 2 * line + 1, 1.0, 0.0).astype(jnp.bfloat16)
    table = scale.astype(jnp.bfloat16)
    half = plan.chunks
    low = jnp.dot(even, table[:, :half], preferred_element_type=jnp.float32)
    high = jnp.dot(odd, table[:, half:], preferred_element_type=jnp.float32)
    return low + high


def two_terms(values):
    high = values.astype(jnp.bfloat16)
    low = (values - high.astype(jnp.float32)).astype(jnp.bfloat16)
    return jnp.concatenate([high, low], axis=1)


def clip_round(values):
    return jnp.clip(values, -quant_limit, quant_limit).astype(jnp.bfloat16)


def turn_matrix(order):
    bits = iota((order, order), 0) & iota((order, order), 1)
    for shift_by in (4, 2, 1):
        bits = bits ^ (bits >> shift_by)
    return (1 - 2 * (bits & 1)).astype(jnp.float32).astype(jnp.bfloat16)


def front(plan, span, mine, activations, out_grads, first_exp, signs):
    first_chunk, chunk_count = span
    group = tile(chunk_count, 8)
    groups = chunk_count // group
    half_rows = plan.rows // 2
    seg = plan.seg_rows
    wide = group * plan.order

    def kernel(acts_hbm, grads_hbm, exp_hbm, signs_hbm, *refs):
        out, (acts_ref, grads_ref, exp_ref, signs_ref, sems) = refs[0], refs[1:]
        copies = [
            pltpu.make_async_copy(signs_hbm, signs_ref, sems.at[0]),
            pltpu.make_async_copy(acts_hbm, acts_ref, sems.at[1]),
            pltpu.make_async_copy(exp_hbm, exp_ref, sems.at[2]),
        ]
        for step in range(groups):
            at = (first_chunk + step * group) * plan.order
            copies.append(
                pltpu.make_async_copy(
                    grads_hbm.at[:, pl.ds(at, wide)], grads_ref.at[step], sems.at[3 + step]
                )
            )
        for copy in copies:
            copy.start()
        outer_place, level, core = places()
        keeper = core if mine else 1 - core
        index = iota((half_rows, 1), 0)
        own = index & (plan.own_rows - 1)
        hop_outer = (index >> log2(plan.own_rows)) & (plan.outer - 1)
        hop_level = index >> log2(seg)
        inner_of = 2 * (level ^ hop_level) + keeper
        row_of = ((outer_place ^ hop_outer) * plan.inner + inner_of) * plan.own_rows + own
        chooser = jnp.where(
            iota((half_rows, plan.rows), 1) == jnp.broadcast_to(row_of, (half_rows, plan.rows)),
            1.0,
            0.0,
        ).astype(jnp.bfloat16)
        root = 1.0 / (plan.order**0.5)
        square = (plan.order, plan.order)
        hadamard = turn_matrix(plan.order)
        for copy in copies:
            copy.wait()
        flips = 1.0 - 2.0 * signs_ref[0:1, :].astype(jnp.float32)
        diagonal = jnp.where(iota(square, 0) == iota(square, 1), flips, 0.0).astype(jnp.bfloat16)
        turn = jnp.dot(diagonal, hadamard, preferred_element_type=jnp.float32).astype(jnp.bfloat16)
        turn = jnp.concatenate([turn, turn], axis=0)
        acts = lax.dot_general(
            chooser, acts_ref[...], (((1,), (1,)), ((), ())), preferred_element_type=jnp.float32
        ).astype(jnp.bfloat16)
        down = pick(plan, row_of, jnp.exp2(-exp_ref[...].astype(jnp.float32))) * root
        for step in range(groups):
            grad = jnp.dot(acts, grads_ref[step], preferred_element_type=jnp.float32)
            stacked = jnp.concatenate(
                [grad[:, c * plan.order : (c + 1) * plan.order] for c in range(group)], axis=0
            )
            rotated = jnp.dot(two_terms(stacked), turn, preferred_element_type=jnp.float32)
            for c in range(group):
                at = first_chunk + step * group + c
                part = rotated[c * half_rows : (c + 1) * half_rows] * down[:, at : at + 1]
                part = clip_round(part)
                for hop in range(plan.levels):
                    row = (hop * chunk_count + step * group + c) * seg
                    out[pl.ds(row, seg), :] = part[hop * seg : (hop + 1) * seg]

    return pl.pallas_call(
        kernel,
        out_shape=jax.ShapeDtypeStruct(
            (plan.levels * chunk_count * seg, plan.order), jnp.bfloat16
        ),
        in_specs=[pl.BlockSpec(memory_space=pltpu.HBM)] * 4,
        out_specs=pl.BlockSpec(memory_space=pltpu.VMEM),
        scratch_shapes=[
            pltpu.VMEM(activations.shape, jnp.bfloat16),
            pltpu.VMEM((groups, plan.tokens, wide), jnp.bfloat16),
            pltpu.VMEM(first_exp.shape, jnp.int32),
            pltpu.VMEM(signs.shape, jnp.int32),
            pltpu.SemaphoreType.DMA((groups + 3,)),
        ],
        compiler_params=vmem(16 if mine or first_chunk else 60),
        name="front_mine" if mine else "front_theirs",
    )(activations, out_grads, first_exp, signs)


def join_cores(plan, ours, theirs):
    rows = ours.shape[0] // plan.levels

    def kernel(one, two, *outs):
        for hop, out in enumerate(outs):
            at = pl.ds(hop * rows, rows)
            total = one[at, :].astype(jnp.float32) + two[at, :].astype(jnp.float32)
            out[...] = total.astype(jnp.bfloat16)

    piece = jax.ShapeDtypeStruct((rows, ours.shape[1]), jnp.bfloat16)
    return pl.pallas_call(
        kernel, out_shape=[piece] * plan.levels, compiler_params=vmem(16), name="join_cores"
    )(ours, theirs)


def add_pieces(one, two):
    def kernel(one_ref, two_ref, out):
        total = one_ref[...].astype(jnp.float32) + two_ref[...].astype(jnp.float32)
        out[...] = total.astype(jnp.bfloat16)

    return pl.pallas_call(
        kernel,
        out_shape=jax.ShapeDtypeStruct(one.shape, one.dtype),
        compiler_params=vmem(8),
        name="add_pieces",
    )(one, two)


def requantize(plan, spans, first_exp, second_exp, parts):
    first_chunk, chunk_count = whole_span(spans)
    seg = plan.seg_rows
    pieces = len(parts[0])

    def kernel(first_ref, second_ref, *refs):
        ins, outs = refs[: pieces * len(spans)], refs[pieces * len(spans) :]
        outer_place, level, core = places()
        index = iota((seg, 1), 0)
        own = index & (plan.own_rows - 1)
        hop = index >> log2(plan.own_rows)
        inner_of = 2 * level + core
        row_of = ((outer_place ^ hop) * plan.inner + inner_of) * plan.own_rows + own
        shift = pick(plan, row_of, jnp.exp2((first_ref[...] - second_ref[...]).astype(jnp.float32)))
        for n, (span_chunk, span_count) in enumerate(spans):
            group = tile(span_count, 16)
            size = group * seg
            here, there = iota((size, size), 0), iota((size, size), 1)
            source = (here & (group - 1)) * seg + (here >> log2(group))
            order = jnp.where(there == source, 1.0, 0.0).astype(jnp.bfloat16)
            for step in range(span_count // group):
                rows = pl.ds(step * size, size)
                total = ins[n * pieces][rows, :].astype(jnp.float32)
                for other in ins[n * pieces + 1 : (n + 1) * pieces]:
                    total = total + other[rows, :].astype(jnp.float32)
                start = span_chunk + step * group
                scaled = jnp.concatenate(
                    [
                        total[c * seg : (c + 1) * seg] * shift[:, start + c : start + c + 1]
                        for c in range(group)
                    ],
                    axis=0,
                )
                moved = jnp.dot(order, clip_round(scaled), preferred_element_type=jnp.float32)
                moved = moved.astype(jnp.bfloat16)
                for m in range(seg):
                    row = (m % plan.own_rows) * chunk_count + start - first_chunk
                    outs[m // plan.own_rows][pl.ds(row, group), :] = moved[
                        m * group : (m + 1) * group
                    ]

    piece = jax.ShapeDtypeStruct((plan.own_rows * chunk_count, plan.order), jnp.bfloat16)
    return pl.pallas_call(
        kernel, out_shape=[piece] * plan.outer, compiler_params=vmem(12), name="requantize"
    )(first_exp, second_exp, *[piece for span_parts in parts for piece in span_parts])


def whole_span(spans):
    return (spans[0][0], sum(count for start, count in spans))


def owner(plan, span, second_exp, third_exp, signs, momentum, parts):
    first_chunk, chunk_count = span
    own_rows, order = plan.own_rows, plan.order
    devices = plan.outer * plan.inner

    def kernel(second_ref, third_ref, signs_ref, momentum_ref, *refs):
        ins, (moment_out, update_out) = refs[: plan.outer], refs[plan.outer :]
        outer_place, level, core = places()
        first_row = (outer_place * plan.inner + 2 * level + core) * own_rows
        row_of = first_row + iota((own_rows, 1), 0)
        diagonal = iota((chunk_count, chunk_count), 0) == iota((chunk_count, chunk_count), 1)

        def column(table):
            chosen = pick(plan, row_of, table)[:, first_chunk : first_chunk + chunk_count]
            return jnp.concatenate(
                [
                    jnp.sum(jnp.where(diagonal, chosen[k : k + 1], 0.0), axis=1, keepdims=True)
                    for k in range(own_rows)
                ],
                axis=0,
            )

        second = second_ref[...].astype(jnp.float32)
        third = third_ref[...].astype(jnp.float32)
        up, third_down, third_up = (column(jnp.exp2(e)) for e in (second, -third, third))
        root = 1.0 / (order**0.5)
        total = ins[0][...].astype(jnp.float32)
        for other in ins[1:]:
            total = total + other[...].astype(jnp.float32)
        flips = 1.0 - 2.0 * signs_ref[...].astype(jnp.float32)
        one, two = flips[0:1, :], flips[1:2, :]
        turn = turn_matrix(order)
        twice = jnp.concatenate([turn, turn], axis=0)
        back = jnp.dot(two_terms(total * up), twice, preferred_element_type=jnp.float32)
        before = jnp.concatenate(
            [
                momentum_ref[pl.ds(k * plan.chunks + first_chunk, chunk_count), :]
                for k in range(own_rows)
            ],
            axis=0,
        )
        moment = momentum_decay * before + back * (one * (root / devices))
        moment_out[...] = moment
        turned = jnp.dot(
            two_terms(moment * (-step_size * two)), twice, preferred_element_type=jnp.float32
        )
        quant = clip_round(turned * (third_down * root))
        restored = jnp.dot(quant, turn, preferred_element_type=jnp.float32)
        update_out[...] = (restored * (third_up * root) * two).astype(jnp.bfloat16)

    shape = (own_rows * chunk_count, order)
    return pl.pallas_call(
        kernel,
        out_shape=[
            jax.ShapeDtypeStruct(shape, jnp.float32),
            jax.ShapeDtypeStruct(shape, jnp.bfloat16),
        ],
        compiler_params=vmem(8),
        name="owner",
    )(second_exp, third_exp, signs, momentum, *parts)


def chip_slab(plan, span, ours, theirs):
    _, chunk_count = span
    own_rows = plan.own_rows
    rows = 2 * own_rows
    group = tile(chunk_count, 16)
    size = group * rows

    def kernel(ours_ref, theirs_ref, out):
        _, _, core = places()
        here, there = iota((size, size), 0), iota((size, size), 1)
        row = here & (rows - 1)
        part = (row >> log2(own_rows)) ^ core
        source = (part * own_rows + (row & (own_rows - 1))) * group + (here >> log2(rows))
        order = jnp.where(there == source, 1.0, 0.0).astype(jnp.bfloat16)
        for step in range(chunk_count // group):
            block = jnp.concatenate(
                [
                    part_ref[pl.ds(k * chunk_count + step * group, group), :]
                    for part_ref in (ours_ref, theirs_ref)
                    for k in range(own_rows)
                ],
                axis=0,
            )
            moved = jnp.dot(order, block, preferred_element_type=jnp.float32).astype(jnp.bfloat16)
            for c in range(group):
                at = (step * group + c) * plan.order
                out[:, pl.ds(at, plan.order)] = moved[c * rows : (c + 1) * rows]

    return pl.pallas_call(
        kernel,
        out_shape=jax.ShapeDtypeStruct((rows, plan.width), jnp.bfloat16),
        compiler_params=vmem(8),
        name="chip_slab",
    )(ours, theirs)


def band_of(level, core):
    return core ^ (level >> 1)


def band_slab(plan, own, near, far):
    def kernel(own_ref, near_ref, far_ref, out):
        _, level, core = places()
        lower, odd = core == 0, (level & 1) == 1
        step = 8 * plan.order
        for at in range(0, plan.width, step):
            cut = pl.ds(at, step)
            near_part = near_ref[:, cut]
            same = jnp.where(lower, own_ref[:, cut], near_part)
            other = jnp.where(lower, near_part, far_ref[:, cut])
            rows = jnp.concatenate(
                [jnp.where(odd, other, same), jnp.where(odd, same, other)], axis=0
            )
            out[:, cut] = rows

    return pl.pallas_call(
        kernel,
        out_shape=jax.ShapeDtypeStruct((plan.slab_rows, plan.width), jnp.bfloat16),
        compiler_params=vmem(8),
        name="band_slab",
    )(own, near, far)


def place_slabs(plan, whole, pieces):
    def kernel(*refs):
        (out, sems), ins = refs[-2:], refs[: len(pieces)]
        outer_place, level, core = places()
        copies = []
        for n, (hop, mine, piece) in enumerate(pieces):
            band = band_of(level, core) if mine else 1 - band_of(level, core)
            row = ((outer_place ^ hop) * 2 + band) * plan.slab_rows
            copies.append(
                pltpu.make_async_copy(ins[n], out.at[pl.ds(row, plan.slab_rows), :], sems.at[n])
            )
        for copy in copies:
            copy.start()
        for copy in copies:
            copy.wait()

    before = [] if whole is None else [whole]
    return pl.pallas_call(
        kernel,
        out_shape=jax.ShapeDtypeStruct((plan.rows, plan.width), jnp.bfloat16),
        in_specs=[pl.BlockSpec(memory_space=pl.ANY)] * (len(pieces) + len(before)),
        out_specs=pl.BlockSpec(memory_space=pl.ANY),
        scratch_shapes=[pltpu.SemaphoreType.DMA((len(pieces),))],
        input_output_aliases={len(pieces): 0} if before else {},
        compiler_params=vmem(8),
        name="place_slabs",
    )(*[piece for hop, mine, piece in pieces], *before)


def send(plan, value, target_of):
    pairs = []
    for o in range(plan.outer):
        for z in range(plan.levels):
            for c in range(2):
                target = target_of(o, z, c)
                if target is not None:
                    to, tz, tc = target
                    pairs.append((o * plan.inner + 2 * z + c, to * plan.inner + 2 * tz + tc))
    return lax.ppermute(value, ("outer", "inner"), pairs)


def swap_cores(plan, value):
    return send(plan, value, lambda o, z, c: (o, z, 1 - c))


def over_levels(plan, value, hop):
    return send(plan, value, lambda o, z, c: (o, z ^ hop, c))


def over_outer(plan, value, hop):
    return send(plan, value, lambda o, z, c: (o ^ hop, z, c))


def to_near(plan, value):
    return send(plan, value, lambda o, z, c: (o, z ^ (2 if c else 1), c))


def to_far(plan, value):
    return send(plan, value, lambda o, z, c: (o, z ^ 3, c) if c else None)


def stream_front(plan, span, activations, out_grads, first_exp, signs):
    theirs = front(plan, span, False, activations, out_grads, first_exp, signs)
    theirs = swap_cores(plan, theirs)
    ours = front(plan, span, True, activations, out_grads, first_exp, signs)
    joined = join_cores(plan, ours, theirs)
    passed = over_levels(plan, joined[3], 1)
    passed = add_pieces(passed, joined[2])
    far = over_levels(plan, passed, 2)
    near = over_levels(plan, joined[1], 1)
    return [joined[0], near, far]


def stream_owner(plan, spans, tables, momentum, parts):
    first_exp, second_exp, third_exp, signs = tables
    span = whole_span(spans)
    parts = requantize(plan, spans, first_exp, second_exp, parts)
    pieces = [parts[0]]
    for hop in range(1, plan.outer):
        pieces.append(over_outer(plan, parts[hop], hop))
    moment, update = owner(plan, span, second_exp, third_exp, signs, momentum, pieces)
    return moment, update, swap_cores(plan, update)


def gather(plan, span, ours, theirs):
    chip = chip_slab(plan, span, ours, theirs)
    near = to_near(plan, chip)
    far = to_far(plan, chip)
    slab = band_slab(plan, chip, near, far)
    mine, other = [slab], []
    for hop in range(1, plan.outer):
        mine.append(over_outer(plan, slab, hop))
    for hop in range(plan.outer):
        other.append(swap_cores(plan, mine[hop]))
    whole = None
    for ready in STAGES:
        whole = place_slabs(
            plan, whole, [p for h in ready for p in ((h, True, mine[h]), (h, False, other[h]))]
        )
    return whole


STAGES = ((0, 3), (2, 1))


def on_device(activations, out_grads, momentum, first_exp, second_exp, third_exp, signs):
    plan = Plan(activations, out_grads, signs, lax.axis_size("outer"), lax.axis_size("inner"))
    if not plan.fits():
        return general(activations, out_grads, momentum, first_exp, second_exp, third_exp, signs)
    exps = [e.reshape(-1, plan.order) for e in (first_exp, second_exp, third_exp)]
    spans = split_chunks(plan.chunks)
    fronts = [stream_front(plan, span, activations, out_grads, exps[0], signs) for span in spans]
    new_momentum, ours, theirs = stream_owner(plan, spans, (*exps, signs), momentum, fronts)
    update = gather(plan, whole_span(spans), ours, theirs)
    return (new_momentum, update)


def split_chunks(chunks):
    first = 5 * chunks // 8
    return [(0, first), (first, chunks - first)]


def solution(mesh):
    in_specs = (
        P(("outer", "inner"), None),
        P(("outer", "inner"), None),
        P(("outer", "inner"), None),
        P(),
        P(),
        P(),
        P(),
    )
    out_specs = (P(("outer", "inner"), None), P())
    return jax.shard_map(
        on_device, mesh=mesh, in_specs=in_specs, out_specs=out_specs, check_vma=False
    )
```

```python
import jax
import jax.numpy as jnp
from jax import lax
from jax.experimental import pallas as pl
from jax.experimental.pallas import tpu as pltpu
from jax.sharding import PartitionSpec as P


quant_limit = 127.0
momentum_decay = 0.9
step_size = 0.5


def hadamard_matrix(order):
    position = jnp.arange(order, dtype=jnp.int32)
    common = jnp.bitwise_and(position[:, None], position[None, :])
    parity = jnp.zeros((order, order), jnp.int32)
    for shift_by in range(order.bit_length() - 1):
        parity = parity + jnp.bitwise_and(jnp.right_shift(common, shift_by), 1)
    return 1.0 - 2.0 * jnp.bitwise_and(parity, 1).astype(jnp.float32)


def rotation(sign_bits):
    order = sign_bits.shape[0]
    flips = 1.0 - 2.0 * sign_bits.astype(jnp.float32)
    return flips[:, None] * hadamard_matrix(order) / jnp.sqrt(jnp.float32(order))


def collect(pieces):
    grouped = lax.all_gather(pieces[None], "outer", axis=0, tiled=True)
    spread = lax.all_gather(grouped, "inner", axis=1, tiled=True)
    return spread.reshape(-1, pieces.shape[1])


def general(activations, out_grads, momentum, first_exp, second_exp, third_exp, signs):
    high = lax.Precision.HIGHEST
    outer_count = lax.axis_size("outer")
    inner_count = lax.axis_size("inner")
    outer_place = lax.axis_index("outer")
    inner_place = lax.axis_index("inner")
    device_count = outer_count * inner_count
    first_rot = rotation(signs[0])
    second_rot = rotation(signs[1])
    grad = lax.dot_general(
        activations, out_grads, (((0,), (0,)), ((), ())), preferred_element_type=jnp.float32
    )
    slab_shape = grad.shape
    order = first_rot.shape[0]
    count_blocks = grad.size // order
    shard_rows = count_blocks // device_count
    rotated = jnp.dot(grad.reshape(count_blocks, order), first_rot, precision=high)
    first_down = jnp.exp2(-first_exp.astype(jnp.float32))[:, None]
    quant_first = jnp.clip(rotated * first_down, -quant_limit, quant_limit).astype(jnp.bfloat16)
    grouped = quant_first.astype(jnp.float32).reshape(outer_count, inner_count * shard_rows, order)
    inner_total = lax.psum_scatter(
        grouped.astype(jnp.bfloat16), "inner", scatter_dimension=1, tiled=True
    ).astype(jnp.float32)
    first_grid = first_exp.reshape(outer_count, inner_count, shard_rows)
    second_grid = second_exp.reshape(outer_count, inner_count, shard_rows)
    third_grid = third_exp.reshape(outer_count, inner_count, shard_rows)
    first_here = lax.dynamic_index_in_dim(first_grid, inner_place, 1, keepdims=False)
    second_here = lax.dynamic_index_in_dim(second_grid, inner_place, 1, keepdims=False)
    shift_scale = jnp.exp2((first_here - second_here).astype(jnp.float32))[:, :, None]
    requant = jnp.clip(inner_total * shift_scale, -quant_limit, quant_limit).astype(jnp.bfloat16)
    total = lax.psum_scatter(
        requant.astype(jnp.float32).astype(jnp.bfloat16), "outer", scatter_dimension=0, tiled=True
    ).astype(jnp.float32)[0]
    second_mine = lax.dynamic_index_in_dim(second_here, outer_place, 0, keepdims=False)
    second_up = jnp.exp2(second_mine.astype(jnp.float32))[:, None]
    mean_grad = jnp.dot(total * second_up, first_rot.T, precision=high) / device_count
    new_momentum = momentum_decay * momentum + mean_grad
    third_row = lax.dynamic_index_in_dim(third_grid, outer_place, 0, keepdims=False)
    third_mine = lax.dynamic_index_in_dim(third_row, inner_place, 0, keepdims=False)
    rotated_step = jnp.dot(-step_size * new_momentum, second_rot, precision=high)
    third_down = jnp.exp2(-third_mine.astype(jnp.float32))[:, None]
    quant_third = jnp.clip(rotated_step * third_down, -quant_limit, quant_limit).astype(
        jnp.bfloat16
    )
    third_up = jnp.exp2(third_mine.astype(jnp.float32))[:, None]
    restored = jnp.dot(quant_third.astype(jnp.float32) * third_up, second_rot.T, precision=high)
    update = collect(restored.astype(jnp.bfloat16)).reshape(slab_shape)
    return (new_momentum, update)


def vmem(mebibytes):
    return pltpu.CompilerParams(vmem_limit_bytes=mebibytes * 1024 * 1024)


def log2(count):
    return count.bit_length() - 1


def tile(count, most):
    return min(count & -count, most)


def power_of_two(count):
    return count > 0 and count & (count - 1) == 0


class Plan:
    def __init__(self, activations, out_grads, signs, outer, inner):
        self.outer, self.inner = outer, inner
        self.levels = inner // 2
        self.tokens, self.rows = activations.shape
        self.order = signs.shape[1]
        self.width = out_grads.shape[1]
        self.chunks = self.width // self.order
        self.own_rows = self.rows // (outer * inner)
        self.seg_rows = outer * self.own_rows
        self.slab_rows = self.levels * self.own_rows

    def fits(self):
        return (
            all(power_of_two(n) for n in (self.outer, self.inner, self.rows, self.chunks))
            and self.levels == 4
            and self.own_rows * self.outer * self.inner == self.rows
            and self.seg_rows == 16
            and self.slab_rows == 16
            and self.outer == 4
            and self.order == 128
            and 2 * self.chunks == self.order
        )


def places():
    outer_place = lax.axis_index("outer")
    inner_place = lax.axis_index("inner")
    return outer_place, inner_place >> 1, inner_place & 1


def iota(shape, axis):
    return lax.broadcasted_iota(jnp.int32, shape, axis)


def pick(plan, row_of, scale):
    count = row_of.shape[0]
    lines = scale.shape[0]
    line = iota((count, lines), 1)
    row_of = jnp.broadcast_to(row_of, (count, lines))
    even = jnp.where(row_of == 2 * line, 1.0, 0.0).astype(jnp.bfloat16)
    odd = jnp.where(row_of == 2 * line + 1, 1.0, 0.0).astype(jnp.bfloat16)
    table = scale.astype(jnp.bfloat16)
    half = plan.chunks
    low = jnp.dot(even, table[:, :half], preferred_element_type=jnp.float32)
    high = jnp.dot(odd, table[:, half:], preferred_element_type=jnp.float32)
    return low + high


def two_terms(values):
    high = values.astype(jnp.bfloat16)
    low = (values - high.astype(jnp.float32)).astype(jnp.bfloat16)
    return jnp.concatenate([high, low], axis=1)


def clip_round(values):
    return jnp.clip(values, -quant_limit, quant_limit).astype(jnp.bfloat16)


def turn_matrix(order):
    bits = iota((order, order), 0) & iota((order, order), 1)
    for shift_by in (4, 2, 1):
        bits = bits ^ (bits >> shift_by)
    return (1 - 2 * (bits & 1)).astype(jnp.float32).astype(jnp.bfloat16)


def front(plan, span, mine, activations, out_grads, first_exp, signs):
    first_chunk, chunk_count = span
    group = tile(chunk_count, 8)
    groups = chunk_count // group
    half_rows = plan.rows // 2
    seg = plan.seg_rows
    wide = group * plan.order
    first = first_chunk == 0 and not mine

    def kernel(acts_hbm, grads_hbm, exp_hbm, signs_hbm, *refs):
        copies = []
        if first:
            out, (acts_ref, grads_ref, exp_ref, signs_ref, sems) = refs[0], refs[1:]
            copies = [
                pltpu.make_async_copy(signs_hbm, signs_ref, sems.at[0]),
                pltpu.make_async_copy(acts_hbm, acts_ref, sems.at[1]),
                pltpu.make_async_copy(exp_hbm, exp_ref, sems.at[2]),
            ]
            for step in range(groups):
                at = (first_chunk + step * group) * plan.order
                copies.append(
                    pltpu.make_async_copy(
                        grads_hbm.at[:, pl.ds(at, wide)], grads_ref.at[step], sems.at[3 + step]
                    )
                )
        else:
            out = refs[0]
            acts_ref, exp_ref, signs_ref = acts_hbm, exp_hbm, signs_hbm
        for copy in copies:
            copy.start()
        late = 3 + (groups + 1) // 2
        outer_place, level, core = places()
        keeper = core if mine else 1 - core
        index = iota((half_rows, 1), 0)
        own = index & (plan.own_rows - 1)
        hop_outer = (index >> log2(plan.own_rows)) & (plan.outer - 1)
        hop_level = index >> log2(seg)
        inner_of = 2 * (level ^ hop_level) + keeper
        row_of = ((outer_place ^ hop_outer) * plan.inner + inner_of) * plan.own_rows + own
        chooser = jnp.where(
            iota((half_rows, plan.rows), 1) == jnp.broadcast_to(row_of, (half_rows, plan.rows)),
            1.0,
            0.0,
        ).astype(jnp.bfloat16)
        root = 1.0 / (plan.order**0.5)
        square = (plan.order, plan.order)
        hadamard = turn_matrix(plan.order)
        for copy in copies[:late]:
            copy.wait()
        flips = 1.0 - 2.0 * signs_ref[0:1, :].astype(jnp.float32)
        diagonal = jnp.where(iota(square, 0) == iota(square, 1), flips, 0.0).astype(jnp.bfloat16)
        turn = jnp.dot(diagonal, hadamard, preferred_element_type=jnp.float32).astype(jnp.bfloat16)
        turn = jnp.concatenate([turn, turn], axis=0)
        acts = lax.dot_general(
            chooser, acts_ref[...], (((1,), (1,)), ((), ())), preferred_element_type=jnp.float32
        ).astype(jnp.bfloat16)
        down = pick(plan, row_of, jnp.exp2(-exp_ref[...].astype(jnp.float32))) * root
        for step in range(groups):
            if first and step == late - 3:
                for copy in copies[late:]:
                    copy.wait()
            if first:
                block = grads_ref[step]
            else:
                at = (first_chunk + step * group) * plan.order
                block = grads_hbm[:, at : at + wide]
            grad = jnp.dot(acts, block, preferred_element_type=jnp.float32)
            stacked = jnp.concatenate(
                [grad[:, c * plan.order : (c + 1) * plan.order] for c in range(group)], axis=0
            )
            rotated = jnp.dot(two_terms(stacked), turn, preferred_element_type=jnp.float32)
            for c in range(group):
                at = first_chunk + step * group + c
                part = rotated[c * half_rows : (c + 1) * half_rows] * down[:, at : at + 1]
                part = clip_round(part)
                for hop in range(plan.levels):
                    row = (hop * chunk_count + step * group + c) * seg
                    out[pl.ds(row, seg), :] = part[hop * seg : (hop + 1) * seg]

    return pl.pallas_call(
        kernel,
        out_shape=jax.ShapeDtypeStruct(
            (plan.levels * chunk_count * seg, plan.order), jnp.bfloat16
        ),
        in_specs=[pl.BlockSpec(memory_space=pltpu.HBM if first else pltpu.VMEM)] * 4,
        out_specs=pl.BlockSpec(memory_space=pltpu.VMEM),
        scratch_shapes=[
            pltpu.VMEM(activations.shape, jnp.bfloat16),
            pltpu.VMEM((groups, plan.tokens, wide), jnp.bfloat16),
            pltpu.VMEM(first_exp.shape, jnp.int32),
            pltpu.VMEM(signs.shape, jnp.int32),
            pltpu.SemaphoreType.DMA((groups + 3,)),
        ]
        if first
        else [],
        compiler_params=vmem(60 if first else 16),
        name="front_mine" if mine else "front_theirs",
    )(activations, out_grads, first_exp, signs)


def join_cores(plan, ours, theirs):
    rows = ours.shape[0] // plan.levels

    def kernel(one, two, *outs):
        for hop, out in enumerate(outs):
            at = pl.ds(hop * rows, rows)
            total = one[at, :].astype(jnp.float32) + two[at, :].astype(jnp.float32)
            out[...] = total.astype(jnp.bfloat16)

    piece = jax.ShapeDtypeStruct((rows, ours.shape[1]), jnp.bfloat16)
    return pl.pallas_call(
        kernel, out_shape=[piece] * plan.levels, compiler_params=vmem(16), name="join_cores"
    )(ours, theirs)


def add_pieces(one, two):
    def kernel(one_ref, two_ref, out):
        total = one_ref[...].astype(jnp.float32) + two_ref[...].astype(jnp.float32)
        out[...] = total.astype(jnp.bfloat16)

    return pl.pallas_call(
        kernel,
        out_shape=jax.ShapeDtypeStruct(one.shape, one.dtype),
        compiler_params=vmem(8),
        name="add_pieces",
    )(one, two)


def scales(plan, span, first_exp, second_exp, third_exp):
    first_chunk, chunk_count = span
    own_rows, seg, order = plan.own_rows, plan.seg_rows, plan.order

    def kernel(first_ref, second_ref, third_ref, shift_out, up_out, down_out, restore_out):
        outer_place, level, core = places()
        index = iota((seg, 1), 0)
        hop = index >> log2(own_rows)
        row_of = ((outer_place ^ hop) * plan.inner + 2 * level + core) * own_rows
        row_of = row_of + (index & (own_rows - 1))
        first = first_ref[...].astype(jnp.float32)
        second = second_ref[...].astype(jnp.float32)
        third = third_ref[...].astype(jnp.float32)
        shift_out[...] = pick(plan, row_of, jnp.exp2(first - second))
        first_row = (outer_place * plan.inner + 2 * level + core) * own_rows
        row_of = first_row + iota((own_rows, 1), 0)
        diagonal = iota((chunk_count, chunk_count), 0) == iota((chunk_count, chunk_count), 1)
        root = 1.0 / (order**0.5)
        for table, factor, out in (
            (jnp.exp2(second), 1.0, up_out),
            (jnp.exp2(-third), root, down_out),
            (jnp.exp2(third), root, restore_out),
        ):
            chosen = pick(plan, row_of, table)[:, first_chunk : first_chunk + chunk_count]
            for k in range(own_rows):
                column = jnp.sum(
                    jnp.where(diagonal, chosen[k : k + 1], 0.0), axis=1, keepdims=True
                )
                out[pl.ds(k * chunk_count, chunk_count), :] = jnp.broadcast_to(
                    column * factor, (chunk_count, order)
                )

    spread = jax.ShapeDtypeStruct((own_rows * chunk_count, order), jnp.float32)
    return pl.pallas_call(
        kernel,
        out_shape=[jax.ShapeDtypeStruct((seg, plan.chunks), jnp.float32)] + [spread] * 3,
        compiler_params=vmem(8),
        name="scales",
    )(first_exp, second_exp, third_exp)


def requantize(plan, spans, shift, parts):
    first_chunk, chunk_count = whole_span(spans)
    seg = plan.seg_rows
    pieces = len(parts[0])

    def kernel(shift_ref, *refs):
        ins, outs = refs[: pieces * len(spans)], refs[pieces * len(spans) :]
        shift = shift_ref[...]
        for n, (span_chunk, span_count) in enumerate(spans):
            group = tile(span_count, 16)
            size = group * seg
            here, there = iota((size, size), 0), iota((size, size), 1)
            source = (here & (group - 1)) * seg + (here >> log2(group))
            order = jnp.where(there == source, 1.0, 0.0).astype(jnp.bfloat16)
            for step in range(span_count // group):
                rows = pl.ds(step * size, size)
                total = ins[n * pieces][rows, :].astype(jnp.float32)
                for other in ins[n * pieces + 1 : (n + 1) * pieces]:
                    total = total + other[rows, :].astype(jnp.float32)
                start = span_chunk + step * group
                scaled = jnp.concatenate(
                    [
                        total[c * seg : (c + 1) * seg] * shift[:, start + c : start + c + 1]
                        for c in range(group)
                    ],
                    axis=0,
                )
                moved = jnp.dot(order, clip_round(scaled), preferred_element_type=jnp.float32)
                moved = moved.astype(jnp.bfloat16)
                for m in range(seg):
                    row = (m % plan.own_rows) * chunk_count + start - first_chunk
                    outs[m // plan.own_rows][pl.ds(row, group), :] = moved[
                        m * group : (m + 1) * group
                    ]

    piece = jax.ShapeDtypeStruct((plan.own_rows * chunk_count, plan.order), jnp.bfloat16)
    return pl.pallas_call(
        kernel, out_shape=[piece] * plan.outer, compiler_params=vmem(12), name="requantize"
    )(shift, *[piece for span_parts in parts for piece in span_parts])


def whole_span(spans):
    return (spans[0][0], sum(count for start, count in spans))


def owner(plan, span, up, down, restore, signs, momentum, parts):
    first_chunk, chunk_count = span
    own_rows, order = plan.own_rows, plan.order
    devices = plan.outer * plan.inner

    def kernel(up_ref, down_ref, restore_ref, signs_ref, momentum_ref, *refs):
        ins, (moment_out, update_out) = refs[: plan.outer], refs[plan.outer :]
        root = 1.0 / (order**0.5)
        total = ins[0][...].astype(jnp.float32)
        for other in ins[1:]:
            total = total + other[...].astype(jnp.float32)
        flips = 1.0 - 2.0 * signs_ref[...].astype(jnp.float32)
        one, two = flips[0:1, :], flips[1:2, :]
        turn = turn_matrix(order)
        twice = jnp.concatenate([turn, turn], axis=0)
        back = jnp.dot(two_terms(total * up_ref[...]), twice, preferred_element_type=jnp.float32)
        before = jnp.concatenate(
            [
                momentum_ref[pl.ds(k * plan.chunks + first_chunk, chunk_count), :]
                for k in range(own_rows)
            ],
            axis=0,
        )
        moment = momentum_decay * before + back * (one * (root / devices))
        moment_out[...] = moment
        turned = jnp.dot(
            two_terms(moment * (-step_size * two)), twice, preferred_element_type=jnp.float32
        )
        quant = clip_round(turned * down_ref[...])
        restored = jnp.dot(quant, turn, preferred_element_type=jnp.float32)
        update_out[...] = (restored * restore_ref[...] * two).astype(jnp.bfloat16)

    shape = (own_rows * chunk_count, order)
    return pl.pallas_call(
        kernel,
        out_shape=[
            jax.ShapeDtypeStruct(shape, jnp.float32),
            jax.ShapeDtypeStruct(shape, jnp.bfloat16),
        ],
        compiler_params=vmem(8),
        name="owner",
    )(up, down, restore, signs, momentum, *parts)


def chip_slab(plan, span, ours, theirs):
    _, chunk_count = span
    own_rows = plan.own_rows
    rows = 2 * own_rows
    group = tile(chunk_count, 16)
    size = group * rows

    def kernel(ours_ref, theirs_ref, out):
        _, _, core = places()
        here, there = iota((size, size), 0), iota((size, size), 1)
        row = here & (rows - 1)
        part = (row >> log2(own_rows)) ^ core
        source = (part * own_rows + (row & (own_rows - 1))) * group + (here >> log2(rows))
        order = jnp.where(there == source, 1.0, 0.0).astype(jnp.bfloat16)
        for step in range(chunk_count // group):
            block = jnp.concatenate(
                [
                    part_ref[pl.ds(k * chunk_count + step * group, group), :]
                    for part_ref in (ours_ref, theirs_ref)
                    for k in range(own_rows)
                ],
                axis=0,
            )
            moved = jnp.dot(order, block, preferred_element_type=jnp.float32).astype(jnp.bfloat16)
            for c in range(group):
                at = (step * group + c) * plan.order
                out[:, pl.ds(at, plan.order)] = moved[c * rows : (c + 1) * rows]

    return pl.pallas_call(
        kernel,
        out_shape=jax.ShapeDtypeStruct((rows, plan.width), jnp.bfloat16),
        compiler_params=vmem(8),
        name="chip_slab",
    )(ours, theirs)


def band_of(level, core):
    return core ^ (level >> 1)


def band_slab(plan, own, near, far):
    def kernel(own_ref, near_ref, far_ref, out):
        _, level, core = places()
        lower, odd = core == 0, (level & 1) == 1
        step = 8 * plan.order
        for at in range(0, plan.width, step):
            cut = pl.ds(at, step)
            near_part = near_ref[:, cut]
            same = jnp.where(lower, own_ref[:, cut], near_part)
            other = jnp.where(lower, near_part, far_ref[:, cut])
            rows = jnp.concatenate(
                [jnp.where(odd, other, same), jnp.where(odd, same, other)], axis=0
            )
            out[:, cut] = rows

    return pl.pallas_call(
        kernel,
        out_shape=jax.ShapeDtypeStruct((plan.slab_rows, plan.width), jnp.bfloat16),
        compiler_params=vmem(8),
        name="band_slab",
    )(own, near, far)


def place_slabs(plan, whole, pieces):
    def kernel(*refs):
        (out, sems), ins = refs[-2:], refs[: len(pieces)]
        outer_place, level, core = places()
        copies = []
        for n, (hop, mine, piece) in enumerate(pieces):
            band = band_of(level, core) if mine else 1 - band_of(level, core)
            row = ((outer_place ^ hop) * 2 + band) * plan.slab_rows
            copies.append(
                pltpu.make_async_copy(ins[n], out.at[pl.ds(row, plan.slab_rows), :], sems.at[n])
            )
        for copy in copies:
            copy.start()
        for copy in copies:
            copy.wait()

    before = [] if whole is None else [whole]
    return pl.pallas_call(
        kernel,
        out_shape=jax.ShapeDtypeStruct((plan.rows, plan.width), jnp.bfloat16),
        in_specs=[pl.BlockSpec(memory_space=pl.ANY)] * (len(pieces) + len(before)),
        out_specs=pl.BlockSpec(memory_space=pl.ANY),
        scratch_shapes=[pltpu.SemaphoreType.DMA((len(pieces),))],
        input_output_aliases={len(pieces): 0} if before else {},
        compiler_params=vmem(8),
        name="place_slabs",
    )(*[piece for hop, mine, piece in pieces], *before)


def send(plan, value, target_of):
    pairs = []
    for o in range(plan.outer):
        for z in range(plan.levels):
            for c in range(2):
                target = target_of(o, z, c)
                if target is not None:
                    to, tz, tc = target
                    pairs.append((o * plan.inner + 2 * z + c, to * plan.inner + 2 * tz + tc))
    return lax.ppermute(value, ("outer", "inner"), pairs)


def swap_cores(plan, value):
    return send(plan, value, lambda o, z, c: (o, z, 1 - c))


def over_levels(plan, value, hop):
    return send(plan, value, lambda o, z, c: (o, z ^ hop, c))


def over_outer(plan, value, hop):
    return send(plan, value, lambda o, z, c: (o ^ hop, z, c))


def to_near(plan, value):
    return send(plan, value, lambda o, z, c: (o, z ^ (2 if c else 1), c))


def to_far(plan, value):
    return send(plan, value, lambda o, z, c: (o, z ^ 3, c) if c else None)


def stream_front(plan, span, activations, out_grads, first_exp, signs):
    theirs = front(plan, span, False, activations, out_grads, first_exp, signs)
    theirs = swap_cores(plan, theirs)
    ours = front(plan, span, True, activations, out_grads, first_exp, signs)
    joined = join_cores(plan, ours, theirs)
    passed = over_levels(plan, joined[3], 1)
    passed = add_pieces(passed, joined[2])
    far = over_levels(plan, passed, 2)
    near = over_levels(plan, joined[1], 1)
    return [joined[0], near, far]


def stream_owner(plan, spans, tables, momentum, parts):
    first_exp, second_exp, third_exp, signs = tables
    span = whole_span(spans)
    shift, up, down, restore = scales(plan, span, first_exp, second_exp, third_exp)
    parts = requantize(plan, spans, shift, parts)
    pieces = [parts[0]]
    for hop in range(1, plan.outer):
        pieces.append(over_outer(plan, parts[hop], hop))
    moment, update = owner(plan, span, up, down, restore, signs, momentum, pieces)
    return moment, update, swap_cores(plan, update)


def gather(plan, span, ours, theirs):
    chip = chip_slab(plan, span, ours, theirs)
    near = to_near(plan, chip)
    far = to_far(plan, chip)
    slab = band_slab(plan, chip, near, far)
    mine, other = [slab], []
    for hop in range(1, plan.outer):
        mine.append(over_outer(plan, slab, hop))
    for hop in range(plan.outer):
        other.append(swap_cores(plan, mine[hop]))
    whole = None
    for ready in STAGES:
        whole = place_slabs(
            plan, whole, [p for h in ready for p in ((h, True, mine[h]), (h, False, other[h]))]
        )
    return whole


STAGES = ((0,), (1,), (2, 3))


def on_device(activations, out_grads, momentum, first_exp, second_exp, third_exp, signs):
    plan = Plan(activations, out_grads, signs, lax.axis_size("outer"), lax.axis_size("inner"))
    if not plan.fits():
        return general(activations, out_grads, momentum, first_exp, second_exp, third_exp, signs)
    exps = [e.reshape(-1, plan.order) for e in (first_exp, second_exp, third_exp)]
    spans = split_chunks(plan.chunks)
    fronts = [stream_front(plan, span, activations, out_grads, exps[0], signs) for span in spans]
    new_momentum, ours, theirs = stream_owner(plan, spans, (*exps, signs), momentum, fronts)
    update = gather(plan, whole_span(spans), ours, theirs)
    return (new_momentum, update)


def split_chunks(chunks):
    first = 9 * chunks // 16
    return [(0, first), (first, chunks - first)]


def solution(mesh):
    in_specs = (
        P(("outer", "inner"), None),
        P(("outer", "inner"), None),
        P(("outer", "inner"), None),
        P(),
        P(),
        P(),
        P(),
    )
    out_specs = (P(("outer", "inner"), None), P())
    return jax.shard_map(
        on_device, mesh=mesh, in_specs=in_specs, out_specs=out_specs, check_vma=False
    )
```
